32 devices in a mesh: space: 8 (over y, x, core), mem: 4 (over z).
Axes of the slice: x: 2, y: 2, z: 4, core: 2. Of those that a mesh axis runs over, the one named last changes fastest.
Arguments:
- increment: float32 [16, 65536], P(None, 'space'), may hold values from -6 to 6
- anomalies: bfloat16 [32, 16, 65536], P('mem', None, 'space'), may hold values from -6 to 6
- interp_index: int32 [3, 65536], P(None, 'space'), may hold values from 0 to 2302, as said below
- interp_weight: float32 [3, 65536], P(None, 'space'), may hold values from 0.2 to 1
- neighbour_blocks: int32 [9, 128], P(None, 'space'), may hold values from 0 to 31, as said below
- tiles: bfloat16 [128, 9, 128, 128], P('space'), may hold values from -0.1875 to 0.1875
Outputs:
- covariance_image: float32 [16, 65536], P(None, ('space', 'mem'))
The draws below stay inside these ranges and needn't reach their ends.
Inputs may be any that keep to these rules, and one draw needn't show every extreme that they name: `interp_index`: column j of a patch, at position i = j % 8192, names points from c - 128 to c + 127, where c = 128 + i * 2048 // 8192. `neighbour_blocks`: row 0 names the block itself (8 plus its place in the patch); the others lie within 8 blocks of it.
All inputs are finite; a program needn't handle non-finite values.
Results may differ from the reference program's by a relative error of at most 0.015.
Values may be sent and summed in bfloat16 or wider, within the bound.
No kernel may reach another device: no remote copies, remote signals or barrier semaphores. Data moves between devices by JAX's collectives and lax.ppermute only.
A program may use at most 64 MiB of HBM per device.

```python
import jax
import jax.numpy as jnp
from jax import lax

LEV = 8
VAR = 2
COLS_DEV = 8192
BLOCK = 128
NB = 9
HI = 128
INTP = 3
SUB_DEV = 2048
HB = 8
HS = 1024
MEMBERS = 32
COLS = 65536
SUBS = 16384
NBLKS = 128


def draw_interp_index(key, part):
    position = jnp.arange(COLS, dtype=jnp.int32) % COLS_DEV
    centre = HI + position * SUB_DEV // COLS_DEV
    offset = jax.random.randint(key, (INTP, COLS), -HI, HI, dtype=jnp.int32)
    return (centre[None, :] + offset).astype(jnp.int32)


def draw_neighbour_blocks(key, part):
    itself = jnp.arange(NBLKS, dtype=jnp.int32) % (SUB_DEV // BLOCK) + HB
    offset = jax.random.randint(key, (NB, NBLKS), -HB, HB + 1, dtype=jnp.int32)
    offset = offset.at[0].set(0)
    return (itself[None, :] + offset).astype(jnp.int32)


def block_levels(stream_key, shape, split, smallest, high):
    loudness = 1.0
    for axis_at, parts in split:
        heights = jax.random.uniform(jax.random.fold_in(jax.random.fold_in(stream_key, 6), axis_at), (parts,), jnp.float32, smallest / len(split), high / len(split))
        loudness = loudness * jnp.repeat(jnp.exp(heights), shape[axis_at] // parts).reshape((-1,) + (1,) * (len(shape) - 1 - axis_at))
    return loudness


def scatter_about(stream_key, dims, deviation, reach, shards=(), kind=jnp.bfloat16):
    drawn = deviation * jax.random.normal(stream_key, dims, jnp.float32)
    if shards:
        drawn = drawn * block_levels(stream_key, dims, shards, -0.22, 0.18)
    return jnp.clip(drawn, -reach, reach).astype(kind)


def setup_inputs(seed: int = 0) -> dict:
    seeds = jax.random.split(jax.random.key(seed), 7)
    return {
        "increment": scatter_about(seeds[0], (LEV * VAR, COLS), 1.0, 6.0, ((1, 8),), jnp.float32),
        "anomalies": scatter_about(seeds[1], (MEMBERS, LEV * VAR, COLS), 1.0, 6.0, ((0, 4), (2, 8))),
        "interp_index": draw_interp_index(jax.random.fold_in(seeds[6], 71), 0),
        "interp_weight": jnp.clip(0.2 + 0.8 * jax.random.uniform(seeds[3], (INTP, COLS), jnp.float32) ** block_levels(seeds[3], (INTP, COLS), ((1, 8),), -0.2, 0.2), 0.2, 1.0),
        "neighbour_blocks": draw_neighbour_blocks(jax.random.fold_in(seeds[6], 71), 0),
        "tiles": scatter_about(seeds[5], (NBLKS, NB, BLOCK, BLOCK), (NB * BLOCK) ** -0.5, 0.1875, ((0, 8),)),
    }


def reference(increment, anomalies, interp_index, interp_weight, neighbour_blocks, tiles):
    n_fields = increment.shape[0]
    blocks_dev = SUB_DEV // BLOCK
    column_patch = jnp.arange(COLS, dtype=jnp.int32) // COLS_DEV
    point_index = (column_patch[None, :] * SUB_DEV + interp_index).astype(jnp.int32)
    block_patch = jnp.arange(NBLKS, dtype=jnp.int32) // blocks_dev
    block_index = (block_patch[None, :] * blocks_dev + neighbour_blocks).astype(jnp.int32)
    tiles_wide = tiles.astype(jnp.float32)

    def member(summed, anomaly):
        weighted = anomaly.astype(jnp.float32) * increment
        spread = jnp.zeros((n_fields, SUBS + 2 * HI), jnp.float32)
        spread = spread.at[:, point_index].add(weighted[:, None, :] * interp_weight[None])
        sub_values = spread[:, HI:HI + SUBS].astype(jnp.bfloat16)
        padded = jnp.pad(sub_values, ((0, 0), (HS, HS)))
        blocked = padded.reshape(n_fields, NBLKS + 2 * HB, BLOCK)
        picked = blocked[:, block_index, :].astype(jnp.float32)
        smooth = jnp.einsum("fnbk,bnkl->fbl", picked, tiles_wide, precision=lax.Precision.HIGHEST)
        smooth = smooth.reshape(n_fields, SUBS).astype(jnp.bfloat16)
        widened = jnp.pad(smooth, ((0, 0), (HI, HI)))
        returned = jnp.sum(widened[:, point_index].astype(jnp.float32) * interp_weight[None], axis=1)
        return summed + anomaly.astype(jnp.float32) * returned, None

    start = jnp.zeros((n_fields, COLS), jnp.float32)
    summed, unused = lax.scan(member, start, anomalies)
    return summed / (MEMBERS - 1)
```

```python
import functools

import jax
import jax.numpy as jnp
from jax import lax
from jax.experimental import pallas as pl
from jax.experimental.pallas import tpu as pltpu
from jax.sharding import PartitionSpec as P

BLOCK = 128
HI = 128
INTP = 3
RATIO = 4
CHUNK = RATIO * BLOCK
WIN = 3 * BLOCK
REACH = 2 * HI + 32
F32 = jnp.float32
BF16 = jnp.bfloat16


def params(kib):
    return pltpu.CompilerParams(vmem_limit_bytes=kib * 1024)


def cost(flops, nbytes):
    return pl.CostEstimate(flops=flops, bytes_accessed=nbytes, transcendentals=0)


def build_table(local, weight, table_ref):
    i0, i1, i2 = local[0:1], local[1:2], local[2:3]
    w0, w1, w2 = weight[0:1], weight[1:2], weight[2:3]
    zero = jnp.zeros_like(w0)
    w0 = w0 + jnp.where(i1 == i0, w1, zero) + jnp.where(i2 == i0, w2, zero)
    w1 = w1 + jnp.where(i2 == i1, w2, zero)
    rows = REACH // 16
    iota = lax.broadcasted_iota(jnp.int32, (rows, 16, BLOCK), 0) * 16 + lax.broadcasted_iota(
        jnp.int32, (rows, 16, BLOCK), 1
    )
    iota = iota.astype(jnp.int16)
    for s in range(CHUNK // BLOCK):
        cols = slice(s * BLOCK, (s + 1) * BLOCK)
        base = s * BLOCK // RATIO

        def wide(x, kind):
            return jnp.broadcast_to(x[:, cols], (16, BLOCK)).astype(kind)[None]

        table = jnp.zeros((1, 16, BLOCK), BF16)
        for index, value in ((i2, w2), (i1, w1), (i0, w0)):
            table = jnp.where(wide(index - base, jnp.int16) == iota, wide(value, BF16), table)
        table_ref[base : base + REACH, cols] = table.reshape(REACH, BLOCK)
        if base:
            table_ref[0:base, cols] = jnp.zeros((base, BLOCK), BF16)
        if base + REACH < WIN:
            table_ref[base + REACH : WIN, cols] = jnp.zeros((WIN - base - REACH, BLOCK), BF16)


def spread_kernel(steps, first, last, flip_ref, anom_ref, incr_ref, index_ref, weight_ref, *rest):
    if first:
        table_ref, out_ref, carry_ref, acc_ref = rest
    else:
        carry_ref, _, table_ref, out_ref, acc_ref = rest
    i = pl.program_id(0)
    flip = flip_ref[0]
    chunks = flip_ref[1]
    done = flip_ref[2]
    step = i + done
    c = jnp.where(flip == 1, chunks - 1 - step, step)

    @pl.when(i == 0)
    def _():
        if first:
            acc_ref[0:2] = jnp.zeros((2,) + acc_ref.shape[1:], F32)
        else:
            acc_ref[0:2] = carry_ref[...]

    build_table(index_ref[...] - c * BLOCK, weight_ref[...], table_ref.at[0])
    rows = acc_ref.shape[1]
    weighted = (anom_ref[...].astype(F32) * incr_ref[...][None]).astype(BF16).reshape(rows, CHUNK)
    window = lax.dot_general(
        weighted, table_ref[0], (((1,), (1,)), ((), ())), preferred_element_type=F32
    )
    acc_ref[2] = jnp.zeros(acc_ref.shape[1:], F32)
    for k in range(3):
        slot = jnp.where(flip == 1, 2 - k, k)
        acc_ref[slot] += window[:, k * BLOCK : (k + 1) * BLOCK]
    total = steps if first else steps + 2
    out_ref[jnp.where(flip == 1, total - 1 - i, i)] = acc_ref[0].astype(BF16)
    acc_ref[0] = acc_ref[1]
    acc_ref[1] = acc_ref[2]

    @pl.when(i == steps - 1)
    def _():
        if first:
            carry_ref[...] = acc_ref[0:2]
        else:
            out_ref[jnp.where(flip == 1, 1, steps)] = acc_ref[0].astype(BF16)
            out_ref[jnp.where(flip == 1, 0, steps + 1)] = acc_ref[1].astype(BF16)


def spread_call(steps, first, info, anomalies, increment, index, weight, carry=None):
    members, fields, columns = anomalies.shape
    rows = members * fields
    chunks = columns // CHUNK

    def at(i, info):
        step = i + info[2]
        return jnp.where(info[0] == 1, chunks - 1 - step, step)

    in_specs = [
        pl.BlockSpec((members, fields, CHUNK), lambda i, info: (0, 0, at(i, info))),
        pl.BlockSpec((fields, CHUNK), lambda i, info: (0, at(i, info))),
        pl.BlockSpec((INTP, CHUNK), lambda i, info: (0, at(i, info))),
        pl.BlockSpec((INTP, CHUNK), lambda i, info: (0, at(i, info))),
    ]
    operands = [anomalies, increment, index, weight]
    blocks = steps if first else steps + 2
    out_shape = [
        jax.ShapeDtypeStruct((chunks, WIN, CHUNK), BF16),
        jax.ShapeDtypeStruct((blocks, rows, BLOCK), BF16),
    ]
    out_specs = [
        pl.BlockSpec((1, WIN, CHUNK), lambda i, info: (at(i, info), 0, 0)),
        pl.BlockSpec((blocks, rows, BLOCK), lambda i, info: (0, 0, 0)),
    ]
    aliases = {}
    if first:
        out_shape.append(jax.ShapeDtypeStruct((2, rows, BLOCK), F32))
        out_specs.append(pl.BlockSpec((2, rows, BLOCK), lambda i, info: (0, 0, 0)))
    else:
        in_specs.append(pl.BlockSpec((2, rows, BLOCK), lambda i, info: (0, 0, 0)))
        in_specs.append(pl.BlockSpec(memory_space=pl.ANY))
        operands.extend(carry)
        aliases = {len(operands): 0}
    return pl.pallas_call(
        functools.partial(spread_kernel, steps, first, not first),
        grid_spec=pltpu.PrefetchScalarGridSpec(
            num_scalar_prefetch=1,
            grid=(steps,),
            in_specs=in_specs,
            out_specs=out_specs,
            scratch_shapes=[pltpu.VMEM((3, rows, BLOCK), F32)],
        ),
        out_shape=out_shape,
        input_output_aliases=aliases,
        compiler_params=params(16 * 1024),
        cost_estimate=cost(2 * rows * steps * WIN * CHUNK, steps * WIN * CHUNK * 4),
        name="spread_first" if first else "spread_rest",
    )(info, *operands)


def conv_kernel(blocks, half, info_ref, nbr_ref, own_a, own_b, got_a, got_b, tiles_ref, out_ref, wide_ref):
    b = pl.program_id(0)
    flip = info_ref[0]
    has_left = info_ref[3]
    has_right = info_ref[4]
    reach = half - 1

    @pl.when(b == 0)
    def _():
        def fill(low, high, left, right):
            wide_ref[reach - 1 : reach - 1 + half] = low[...]
            wide_ref[reach - 1 + half : reach - 1 + 2 * half] = high[...]
            zeros = jnp.zeros((half,) + wide_ref.shape[1:], BF16)

            @pl.when(has_left == 1)
            def _():
                wide_ref[0 : reach - 1] = left[0 : reach - 1]
                wide_ref[reach - 1 : reach + 1] = (
                    left[reach - 1 : reach + 1].astype(F32) + low[0:2].astype(F32)
                ).astype(BF16)

            @pl.when(has_left == 0)
            def _():
                wide_ref[0:reach] = zeros[0:reach]

            top = blocks + reach

            @pl.when(has_right == 1)
            def _():
                wide_ref[top - 1 : top + 1] = (
                    right[0:2].astype(F32) + high[half - 2 : half].astype(F32)
                ).astype(BF16)
                wide_ref[top + 1 : top + reach] = right[2:half]

            @pl.when(has_right == 0)
            def _():
                wide_ref[top : top + reach] = zeros[0:reach]

        @pl.when(flip == 0)
        def _():
            fill(own_b, own_a, got_b, got_a)

        @pl.when(flip == 1)
        def _():
            fill(own_a, own_b, got_a, got_b)

    count = tiles_ref.shape[1]
    picked = jnp.concatenate([wide_ref[nbr_ref[n, b]] for n in range(count)], axis=1)
    smooth = jnp.dot(
        picked, tiles_ref[0].reshape(count * BLOCK, BLOCK), preferred_element_type=F32
    )
    out_ref[0] = smooth.astype(BF16)


def conv_call(info, neighbours, own_a, own_b, got_a, got_b, tiles):
    blocks, count = tiles.shape[:2]
    half, rows, _ = own_a.shape
    reach = half - 1
    full = pl.BlockSpec((half, rows, BLOCK), lambda b, info, nbr: (0, 0, 0))
    return pl.pallas_call(
        functools.partial(conv_kernel, blocks, half),
        grid_spec=pltpu.PrefetchScalarGridSpec(
            num_scalar_prefetch=2,
            grid=(blocks,),
            in_specs=[full] * 4
            + [pl.BlockSpec((1, count, BLOCK, BLOCK), lambda b, info, nbr: (b, 0, 0, 0))],
            out_specs=pl.BlockSpec((1, rows, BLOCK), lambda b, info, nbr: (b, 0, 0)),
            scratch_shapes=[pltpu.VMEM((blocks + 2 * reach, rows, BLOCK), BF16)],
        ),
        out_shape=jax.ShapeDtypeStruct((blocks, rows, BLOCK), BF16),
        compiler_params=params(16 * 1024),
        cost_estimate=cost(2 * rows * blocks * count * BLOCK * BLOCK, tiles.size * 2),
        name="convolve",
    )(info, neighbours, own_a, own_b, got_a, got_b, tiles)


def back_kernel(info_ref, smooth_ref, got_a, got_b, table_ref, anom_ref, out_ref, own_ref, wide_ref):
    c = pl.program_id(0)
    blocks = smooth_ref.shape[0]
    flip = info_ref[0]

    @pl.when(c == 0)
    def _():
        wide_ref[1 : blocks + 1] = smooth_ref[...]
        left = jnp.where(flip == 1, got_a[...], got_b[...])
        right = jnp.where(flip == 1, got_b[...], got_a[...])
        wide_ref[0] = jnp.where(info_ref[3] == 1, left, jnp.zeros_like(left))
        wide_ref[blocks + 1] = jnp.where(info_ref[4] == 1, right, jnp.zeros_like(right))

    lhs = jnp.concatenate([wide_ref[c], wide_ref[c + 1], wide_ref[c + 2]], axis=1)
    returned = jnp.dot(lhs, table_ref[0], preferred_element_type=F32)
    anom = anom_ref[...].astype(F32)
    value = jnp.sum(anom * returned.reshape(anom.shape), axis=0)
    out_ref[0] = value.astype(BF16)
    shares = info_ref[5]
    per = blocks // shares

    @pl.when(c // per == info_ref[6])
    def _():
        own_ref[c % per] = value


def back_call(info, shares, smooth, got_a, got_b, table, anomalies):
    members, fields, columns = anomalies.shape
    blocks, rows, _ = smooth.shape
    per = blocks // shares
    edge = pl.BlockSpec((rows, BLOCK), lambda c, info: (0, 0))
    return pl.pallas_call(
        back_kernel,
        grid_spec=pltpu.PrefetchScalarGridSpec(
            num_scalar_prefetch=1,
            grid=(blocks,),
            in_specs=[
                pl.BlockSpec((blocks, rows, BLOCK), lambda c, info: (0, 0, 0)),
                edge,
                edge,
                pl.BlockSpec((1, WIN, CHUNK), lambda c, info: (c, 0, 0)),
                pl.BlockSpec((members, fields, CHUNK), lambda c, info: (0, 0, c)),
            ],
            out_specs=[
                pl.BlockSpec((1, fields, CHUNK), lambda c, info: (c, 0, 0)),
                pl.BlockSpec((per, fields, CHUNK), lambda c, info: (0, 0, 0)),
            ],
            scratch_shapes=[pltpu.VMEM((blocks + 2, rows, BLOCK), BF16)],
        ),
        out_shape=[
            jax.ShapeDtypeStruct((blocks, fields, CHUNK), BF16),
            jax.ShapeDtypeStruct((per, fields, CHUNK), F32),
        ],
        compiler_params=params(16 * 1024),
        cost_estimate=cost(2 * rows * blocks * WIN * CHUNK, table.size * 2),
        name="back",
    )(info, smooth, got_a, got_b, table, anomalies)


def swaps(count):
    inner = [(i, i ^ 1) for i in range(count)]
    outer = [(i, (i + 1) % count if i % 2 else (i - 1) % count) for i in range(count)]
    return inner, outer


def shards(increment, anomalies, interp_index, interp_weight, neighbour_blocks, tiles):
    members, fields, columns = anomalies.shape
    chunks = columns // CHUNK
    space = lax.axis_index("space")
    count = lax.axis_size("space")
    mem = lax.axis_index("mem")
    shares = lax.axis_size("mem")
    flip = space % 2
    inner, outer = swaps(count)
    head = chunks // 2 + 1

    def info_of(done):
        return jnp.stack(
            [
                flip,
                jnp.int32(chunks),
                jnp.int32(done),
                (space > 0).astype(jnp.int32),
                (space < count - 1).astype(jnp.int32),
                jnp.int32(shares),
                mem,
            ]
        ).astype(jnp.int32)

    info = info_of(0)
    table, own_b, carry = spread_call(
        head, True, info, anomalies, increment, interp_index, interp_weight
    )
    got_b = lax.ppermute(own_b, "space", outer)
    table, own_a = spread_call(
        chunks - head,
        False,
        info_of(head),
        anomalies,
        increment,
        interp_index,
        interp_weight,
        (carry, table),
    )
    got_a = lax.ppermute(own_a, "space", inner)
    smooth = conv_call(info, neighbour_blocks, own_a, own_b, got_a, got_b, tiles)
    low, high = smooth[0], smooth[chunks - 1]
    edge_a = lax.ppermute(jnp.where(flip == 1, low, high), "space", inner)
    edge_b = lax.ppermute(jnp.where(flip == 1, high, low), "space", outer)
    pieces, own = back_call(info, shares, smooth, edge_a, edge_b, table, anomalies)
    per = chunks // shares
    pieces = pieces.reshape(shares, per, fields, CHUNK)
    total = own
    for shift in range(1, shares):
        piece = lax.dynamic_index_in_dim(pieces, (mem + shift) % shares, 0, False)
        got = lax.ppermute(piece, "mem", [(i, (i + shift) % shares) for i in range(shares)])
        total = total + got.astype(F32)
    total = total / (members * shares - 1)
    return jnp.swapaxes(total, 0, 1).reshape(fields, per * CHUNK)


def solution(mesh):
    in_specs = (
        P(None, "space"),
        P("mem", None, "space"),
        P(None, "space"),
        P(None, "space"),
        P(None, "space"),
        P("space", None, None, None),
    )
    out_specs = P(None, ("space", "mem"))
    return jax.shard_map(shards, mesh=mesh, in_specs=in_specs, out_specs=out_specs, check_vma=False)
```

```python
import functools

import jax
import jax.numpy as jnp
from jax import lax
from jax.experimental import pallas as pl
from jax.experimental.pallas import tpu as pltpu
from jax.sharding import PartitionSpec as P


BLOCK = 128
HI = 128
INTP = 3
RATIO = 4
CHUNK = RATIO * BLOCK
WIN = 3 * BLOCK
REACH = 2 * HI + 32
F32 = jnp.float32
BF16 = jnp.bfloat16
VMEM = pltpu.VMEM
ANY = pl.BlockSpec(memory_space=pl.ANY)
IN_VMEM = pl.BlockSpec(memory_space=pltpu.VMEM)
IN_SMEM = pl.BlockSpec(memory_space=pltpu.SMEM)


def in_hbm(x):
    return pltpu.with_memory_space_constraint(x, pltpu.HBM)


def call(kernel, in_specs, out_specs, out_shape, scratch, flops, aliases=None):
    return pl.pallas_call(
        kernel,
        in_specs=in_specs,
        out_specs=out_specs,
        out_shape=out_shape,
        scratch_shapes=scratch,
        input_output_aliases=aliases or {},
        compiler_params=pltpu.CompilerParams(vmem_limit_bytes=16 * 1024 * 1024),
        cost_estimate=pl.CostEstimate(flops=flops, bytes_accessed=0, transcendentals=0),
    )


def groups(steps, unroll, body):
    unroll = unroll if steps % unroll == 0 else 1

    def group(g, carry):
        for j in range(unroll):
            body(g * unroll + j)
        return carry

    lax.fori_loop(0, steps // unroll, group, 0)


def build_table(local, weight, table_ref):
    i0, i1, i2 = local[0:1], local[1:2], local[2:3]
    w0, w1, w2 = weight[0:1], weight[1:2], weight[2:3]
    zero = jnp.zeros_like(w0)
    w0 = w0 + jnp.where(i1 == i0, w1, zero) + jnp.where(i2 == i0, w2, zero)
    w1 = w1 + jnp.where(i2 == i1, w2, zero)
    rows = REACH // 16
    iota = lax.broadcasted_iota(jnp.int32, (rows, 16, BLOCK), 0) * 16 + lax.broadcasted_iota(
        jnp.int32, (rows, 16, BLOCK), 1
    )
    iota = iota.astype(jnp.int16)
    for s in range(CHUNK // BLOCK):
        cols = slice(s * BLOCK, (s + 1) * BLOCK)
        base = s * BLOCK // RATIO

        def wide(x, kind):
            return jnp.broadcast_to(x[:, cols], (16, BLOCK)).astype(kind)[None]

        table = jnp.zeros((1, 16, BLOCK), BF16)
        for index, value in ((i2, w2), (i1, w1), (i0, w0)):
            table = jnp.where(wide(index - base, jnp.int16) == iota, wide(value, BF16), table)
        table_ref[base : base + REACH, cols] = table.reshape(REACH, BLOCK)
        if base:
            table_ref[0:base, cols] = jnp.zeros((base, BLOCK), BF16)
        if base + REACH < WIN:
            table_ref[base + REACH : WIN, cols] = jnp.zeros((WIN - base - REACH, BLOCK), BF16)


def spread_kernel(steps, done, unroll, chunks, *refs):
    first = done == 0
    if first:
        info_ref, anom_hbm, incr_hbm, index_hbm, weight_hbm = refs[:5]
        table_ref, anom_ref, out_ref, carry_ref = refs[5:9]
        incr_ref, index_ref, weight_ref, acc_ref, anom_sem, incr_sem, some_sem = refs[9:]
    else:
        info_ref, anom_hbm, incr_hbm, index_hbm, weight_hbm, tiles_hbm, carry_ref = refs[:7]
        table_ref, anom_ref, out_ref, tiles_ref = refs[9:13]
        incr_ref, index_ref, weight_ref, acc_ref, anom_sem, incr_sem, some_sem = refs[13:]
    flip = info_ref[0] == 1
    low = jnp.where(flip, chunks - done - steps, done)

    def chunk_of(i):
        return jnp.where(flip, chunks - 1 - done - i, done + i)

    def lanes(c, count=1):
        return pl.ds(pl.multiple_of(c * CHUNK, CHUNK), count * CHUNK)

    index_copy = pltpu.make_async_copy(index_hbm.at[:, lanes(low, steps)], index_ref, some_sem.at[0])
    weight_copy = pltpu.make_async_copy(
        weight_hbm.at[:, lanes(low, steps)], weight_ref, some_sem.at[1]
    )
    index_copy.start()
    weight_copy.start()

    def chunk_copies(i):
        c = chunk_of(i)
        return (
            pltpu.make_async_copy(anom_hbm.at[:, :, lanes(c)], anom_ref.at[c], anom_sem.at[i]),
            pltpu.make_async_copy(incr_hbm.at[:, lanes(c)], incr_ref.at[i], incr_sem.at[i]),
        )

    for i in range(steps):
        for copy in chunk_copies(i):
            copy.start()
    if first:
        acc_ref[...] = jnp.zeros(acc_ref.shape, F32)
    else:
        tiles_copy = pltpu.make_async_copy(tiles_hbm, tiles_ref, some_sem.at[2])
        tiles_copy.start()
        acc_ref[...] = carry_ref[...]
    index_copy.wait()
    weight_copy.wait()
    rows = anom_ref.shape[1] * anom_ref.shape[2]
    total = steps if first else steps + 2

    def group(g, carry):
        acc0, acc1 = acc_ref[0], acc_ref[1]
        steps_here = [g * unroll + j for j in range(unroll)]
        for i in steps_here:
            for copy in chunk_copies(i):
                copy.wait()
        for i in steps_here:
            c = chunk_of(i)
            here = lanes(c - low)
            build_table(index_ref[:, here] - c * BLOCK, weight_ref[:, here], table_ref.at[c])
            weighted = (anom_ref[c].astype(F32) * incr_ref[i][None]).astype(BF16)
            window = lax.dot_general(
                table_ref[c],
                weighted.reshape(rows, CHUNK),
                (((1,), (1,)), ((), ())),
                preferred_element_type=F32,
            )
            near, mid, far = window[:BLOCK], window[BLOCK : 2 * BLOCK], window[2 * BLOCK :]
            ready = acc0 + jnp.where(flip, far, near)
            out_ref[jnp.where(flip, total - 1 - i, i)] = ready.T.astype(BF16)
            acc0 = acc1 + mid
            acc1 = jnp.where(flip, near, far)
        acc_ref[0] = acc0
        acc_ref[1] = acc1
        return carry

    lax.fori_loop(0, steps // unroll, group, 0)
    if first:
        carry_ref[...] = acc_ref[...]
    else:
        out_ref[jnp.where(flip, 1, steps)] = acc_ref[0].T.astype(BF16)
        out_ref[jnp.where(flip, 0, steps + 1)] = acc_ref[1].T.astype(BF16)
        tiles_copy.wait()


def spread_call(steps, done, unroll, info, anomalies, increment, index, weight, extra=()):
    members, fields, columns = anomalies.shape
    rows = members * fields
    chunks = columns // CHUNK
    first = done == 0
    in_specs = [IN_SMEM, ANY, ANY, ANY, ANY]
    out_shape = [
        VMEM((chunks, WIN, CHUNK), BF16),
        VMEM((chunks, members, fields, CHUNK), BF16),
        jax.ShapeDtypeStruct((chunks // 2 + 1, rows, BLOCK), BF16),
    ]
    aliases = {}
    if first:
        out_shape.append(VMEM((2, BLOCK, rows), F32))
    else:
        in_specs += [ANY, IN_VMEM, IN_VMEM, IN_VMEM]
        out_shape.append(VMEM(extra[0].shape, BF16))
        aliases = {7: 0, 8: 1}
    return call(
        functools.partial(spread_kernel, steps, done, unroll, chunks),
        in_specs,
        [IN_VMEM] * 4,
        out_shape,
        [
            VMEM((steps, fields, CHUNK), F32),
            VMEM((INTP, steps * CHUNK), jnp.int32),
            VMEM((INTP, steps * CHUNK), F32),
            VMEM((2, BLOCK, rows), F32),
            pltpu.SemaphoreType.DMA((steps,)),
            pltpu.SemaphoreType.DMA((steps,)),
            pltpu.SemaphoreType.DMA((3,)),
        ],
        2 * rows * steps * WIN * CHUNK,
        aliases,
    )(info, in_hbm(anomalies), in_hbm(increment), in_hbm(index), in_hbm(weight), *extra)


def convolve(wide_ref, tiles_ref, nbr_ref, smooth_ref, b):
    count = tiles_ref.shape[1]
    picked = jnp.concatenate([wide_ref[nbr_ref[n, b]] for n in range(count)], axis=1)
    weights = tiles_ref[b].reshape(count * BLOCK, BLOCK)
    smooth = jnp.dot(picked, weights, preferred_element_type=F32)
    smooth_ref[b + 1] = smooth.astype(BF16)


def conv_early_kernel(
    unroll, info_ref, nbr_ref, own_a, own_b, got_a, tiles_ref, wide_ref, smooth_ref, edge_ref
):
    half = own_a.shape[0]
    reach = half - 1
    blocks = tiles_ref.shape[0]
    top = blocks + reach
    flip = info_ref[0] == 1

    @pl.when(jnp.logical_not(flip))
    def _():
        wide_ref[reach - 1 : reach - 1 + half] = own_b[...]
        wide_ref[reach - 1 + half : top - 1] = own_a[0 : half - 2]
        wide_ref[top - 1 : top + 1] = (
            got_a[0:2].astype(F32) + own_a[half - 2 : half].astype(F32)
        ).astype(BF16)
        wide_ref[top + 1 : top + reach] = got_a[2:half]

    @pl.when(flip)
    def _():
        wide_ref[0 : reach - 1] = got_a[0 : reach - 1]
        wide_ref[reach - 1 : reach + 1] = (
            got_a[reach - 1 : reach + 1].astype(F32) + own_a[0:2].astype(F32)
        ).astype(BF16)
        wide_ref[reach + 1 : reach - 1 + half] = own_a[2:half]
        wide_ref[reach - 1 + half : top + 1] = own_b[...]

    early = blocks - half
    start = jnp.where(flip, 0, half)
    groups(
        early, unroll, lambda i: convolve(wide_ref, tiles_ref, nbr_ref, smooth_ref, start + i)
    )
    edge_ref[...] = smooth_ref[jnp.where(flip, 1, blocks)]


def conv_late_kernel(
    unroll, info_ref, nbr_ref, got_b, tiles_ref, wide_in, smooth_in, wide_ref, smooth_ref, edge_ref
):
    half = got_b.shape[0]
    reach = half - 1
    blocks = tiles_ref.shape[0]
    top = blocks + reach
    flip = info_ref[0] == 1
    present = info_ref[1] == 1
    beyond = jnp.where(present, got_b[...], jnp.zeros(got_b.shape, BF16))

    @pl.when(jnp.logical_not(flip))
    def _():
        wide_ref[0 : reach - 1] = beyond[0 : reach - 1]
        both = wide_ref[reach - 1 : reach + 1].astype(F32) + beyond[reach - 1 :].astype(F32)
        wide_ref[reach - 1] = jnp.where(present, both[0], jnp.zeros_like(both[0])).astype(BF16)
        wide_ref[reach] = both[1].astype(BF16)

    @pl.when(flip)
    def _():
        wide_ref[top + 1 : top + reach] = beyond[2:half]
        both = wide_ref[top - 1 : top + 1].astype(F32) + beyond[0:2].astype(F32)
        wide_ref[top - 1] = both[0].astype(BF16)
        wide_ref[top] = jnp.where(present, both[1], jnp.zeros_like(both[1])).astype(BF16)

    start = jnp.where(flip, blocks - half, 0)
    groups(half, unroll, lambda i: convolve(wide_ref, tiles_ref, nbr_ref, smooth_ref, start + i))
    edge_ref[...] = smooth_ref[jnp.where(flip, blocks, 1)]


def conv_early_call(info, neighbours, own_a, own_b, got_a, tiles):
    blocks, count = tiles.shape[:2]
    half, rows, _ = own_a.shape
    early = blocks - half
    return call(
        functools.partial(conv_early_kernel, early),
        [IN_SMEM, IN_SMEM] + [IN_VMEM] * 4,
        [IN_VMEM] * 3,
        [
            VMEM((blocks + 2 * half - 2, rows, BLOCK), BF16),
            VMEM((blocks + 2, rows, BLOCK), BF16),
            jax.ShapeDtypeStruct((rows, BLOCK), BF16),
        ],
        [],
        2 * rows * early * count * BLOCK * BLOCK,
    )(info, neighbours, own_a, own_b, got_a, tiles)


def conv_late_call(info, neighbours, got_b, tiles, wide, smooth):
    _, count = tiles.shape[:2]
    half, rows, _ = got_b.shape
    return call(
        functools.partial(conv_late_kernel, 3),
        [IN_SMEM, IN_SMEM] + [IN_VMEM] * 4,
        [IN_VMEM] * 3,
        [
            VMEM(wide.shape, BF16),
            VMEM(smooth.shape, BF16),
            jax.ShapeDtypeStruct((rows, BLOCK), BF16),
        ],
        [],
        2 * rows * half * count * BLOCK * BLOCK,
        {4: 0, 5: 1},
    )(info, neighbours, got_b, tiles, wide, smooth)


def back_kernel(part, steps, unroll, per, *refs):
    if part == 0:
        info_ref, got_ref, table_ref, anom_ref, _, smooth_ref, out_ref = refs
    elif part == 1:
        info_ref, table_ref, anom_ref, smooth_ref, _, out_ref = refs
    else:
        info_ref, got_ref, table_ref, anom_ref, _, _, smooth_ref, out_ref = refs
    flip = info_ref[0] == 1
    blocks = table_ref.shape[0]
    if part == 0:
        smooth_ref[jnp.where(flip, 0, blocks + 1)] = got_ref[...]
        start = jnp.where(flip, 0, blocks - steps)
    elif part == 1:
        start = jnp.where(flip, blocks - 1 - steps, 1)
    else:
        got = got_ref[...]
        present = info_ref[1] == 1
        smooth_ref[jnp.where(flip, blocks + 1, 0)] = jnp.where(present, got, jnp.zeros_like(got))
        start = jnp.where(flip, blocks - 1, 0)

    def body(i):
        c = start + i
        lhs = jnp.concatenate([smooth_ref[c], smooth_ref[c + 1], smooth_ref[c + 2]], axis=1)
        returned = jnp.dot(lhs, table_ref[c], preferred_element_type=F32)
        anom = anom_ref[c].astype(F32)
        value = jnp.sum(anom * returned.reshape(anom.shape), axis=0)
        lane = pl.multiple_of(lax.rem(c, per) * CHUNK, CHUNK)
        out_ref[lax.div(c, per), :, pl.ds(lane, CHUNK)] = value.astype(BF16)

    groups(steps, unroll, body)


def back_call(part, steps, unroll, shares, info, got, table, anom, smooth, out=None):
    chunks, members, fields, _ = anom.shape
    per = chunks // shares
    operands = [info] + ([] if part == 1 else [got]) + [table, anom, smooth]
    in_specs = [IN_SMEM] + [IN_VMEM] * (len(operands) - 1)
    out_type = VMEM((shares, fields, per * CHUNK), BF16)
    if part == 2:
        out_type = jax.ShapeDtypeStruct(out_type.shape, BF16)
    smooth_type = VMEM(smooth.shape, BF16)
    last = len(operands) - 1
    if part == 0:
        out_shape, aliases = [smooth_type, out_type], {last: 0}
    elif part == 1:
        operands, in_specs = operands + [out], in_specs + [IN_VMEM]
        out_shape, aliases = [out_type], {last + 1: 0}
    else:
        operands, in_specs = operands + [out], in_specs + [IN_VMEM]
        out_shape, aliases = [smooth_type, out_type], {last: 0, last + 1: 1}
    return call(
        functools.partial(back_kernel, part, steps, unroll, per),
        in_specs,
        [IN_VMEM] * len(out_shape),
        out_shape,
        [],
        2 * members * fields * steps * WIN * CHUNK,
        aliases,
    )(*operands)


def swaps(count):
    inner = [(i, i ^ 1) for i in range(count)]
    outer = [(i, (i + 1) % count if i % 2 else (i - 1) % count) for i in range(count)]
    return inner, outer


def swap(value, pairs):
    return lax.ppermute(value, "space", pairs)


def shards(increment, anomalies, interp_index, interp_weight, neighbour_blocks, tiles):
    members, _, columns = anomalies.shape
    chunks = columns // CHUNK
    space = lax.axis_index("space")
    count = lax.axis_size("space")
    mem = lax.axis_index("mem")
    shares = lax.axis_size("mem")
    assert count % 2 == 0
    flip = space % 2
    inner, outer = swaps(count)
    head = chunks // 2 + 1
    present = jnp.where(flip == 1, space < count - 1, space > 0)
    info = jnp.stack([flip, present.astype(jnp.int32)]).astype(jnp.int32)
    columns_in = (anomalies, increment, interp_index, interp_weight)
    table, anom, own_b, carry = spread_call(head, 0, 3, info, *columns_in)
    got_b = swap(own_b, outer)
    table, anom, own_a, tiles_here = spread_call(
        chunks - head, head, 1, info, *columns_in, (in_hbm(tiles), carry, table, anom)
    )
    got_a = swap(own_a, inner)
    wide, smooth, edge_a = conv_early_call(info, neighbour_blocks, own_a, own_b, got_a, tiles_here)
    halo_a = swap(edge_a, inner)
    smooth, out = back_call(0, chunks - head - 1, 3, shares, info, halo_a, table, anom, smooth)
    wide, smooth, edge_b = conv_late_call(info, neighbour_blocks, got_b, tiles_here, wide, smooth)
    halo_b = swap(edge_b, outer)
    (out,) = back_call(1, head, 3, shares, info, None, table, anom, smooth, out)
    _, pieces = back_call(2, 1, 1, shares, info, halo_b, table, anom, smooth, out)

    def piece_of(share):
        return lax.dynamic_index_in_dim(pieces, share, 0, False)

    total = piece_of(mem).astype(F32)
    for shift in range(1, shares):
        got = lax.ppermute(
            piece_of((mem + shift) % shares),
            "mem",
            [(i, (i + shift) % shares) for i in range(shares)],
        )
        total = total + got.astype(F32)
    return total / (members * shares - 1)


def solution(mesh):
    in_specs = (
        P(None, "space"),
        P("mem", None, "space"),
        P(None, "space"),
        P(None, "space"),
        P(None, "space"),
        P("space", None, None, None),
    )
    out_specs = P(None, ("space", "mem"))
    return jax.shard_map(shards, mesh=mesh, in_specs=in_specs, out_specs=out_specs, check_vma=False)
```

```python
import functools

import jax
import jax.numpy as jnp
from jax import lax
from jax.experimental import pallas as pl
from jax.experimental.pallas import tpu as pltpu
from jax.sharding import PartitionSpec as P


BLOCK = 128
HI = 128
INTP = 3
RATIO = 4
CHUNK = RATIO * BLOCK
WIN = 3 * BLOCK
REACH = 2 * HI + 32
F32 = jnp.float32
BF16 = jnp.bfloat16
VMEM = pltpu.VMEM
ANY = pl.BlockSpec(memory_space=pl.ANY)
IN_VMEM = pl.BlockSpec(memory_space=pltpu.VMEM)
IN_SMEM = pl.BlockSpec(memory_space=pltpu.SMEM)


def in_hbm(x):
    return pltpu.with_memory_space_constraint(x, pltpu.HBM)


def call(kernel, in_specs, out_specs, out_shape, scratch, aliases=None):
    return pl.pallas_call(
        kernel,
        in_specs=in_specs,
        out_specs=out_specs,
        out_shape=out_shape,
        scratch_shapes=scratch,
        input_output_aliases=aliases or {},
        compiler_params=pltpu.CompilerParams(vmem_limit_bytes=16 * 1024 * 1024),
        cost_estimate=pl.CostEstimate(flops=0, bytes_accessed=0, transcendentals=0),
    )


def groups(steps, unroll, body):
    unroll = unroll if steps % unroll == 0 else 1

    def group(g, carry):
        for j in range(unroll):
            body(g * unroll + j)
        return carry

    lax.fori_loop(0, steps // unroll, group, 0)


def build_table(local, weight, table_ref):
    i0, i1, i2 = local[0:1], local[1:2], local[2:3]
    w0, w1, w2 = weight[0:1], weight[1:2], weight[2:3]
    zero = jnp.zeros_like(w0)
    w0 = w0 + jnp.where(i1 == i0, w1, zero) + jnp.where(i2 == i0, w2, zero)
    w1 = w1 + jnp.where(i2 == i1, w2, zero)
    rows = REACH // 16
    iota = lax.broadcasted_iota(jnp.int32, (rows, 16, BLOCK), 0) * 16 + lax.broadcasted_iota(
        jnp.int32, (rows, 16, BLOCK), 1
    )
    iota = iota.astype(jnp.int16)
    for s in range(CHUNK // BLOCK):
        cols = slice(s * BLOCK, (s + 1) * BLOCK)
        base = s * BLOCK // RATIO

        def wide(x, kind):
            return jnp.broadcast_to(x[:, cols], (16, BLOCK)).astype(kind)[None]

        table = jnp.zeros((1, 16, BLOCK), BF16)
        for index, value in ((i2, w2), (i1, w1), (i0, w0)):
            table = jnp.where(wide(index - base, jnp.int16) == iota, wide(value, BF16), table)
        table_ref[base : base + REACH, cols] = table.reshape(REACH, BLOCK)
        if base:
            table_ref[0:base, cols] = jnp.zeros((base, BLOCK), BF16)
        if base + REACH < WIN:
            table_ref[base + REACH : WIN, cols] = jnp.zeros((WIN - base - REACH, BLOCK), BF16)


def spread_kernel(steps, done, unroll, chunks, *refs):
    first = done == 0
    if first:
        info_ref, anom_hbm, incr_hbm, index_hbm, weight_hbm = refs[:5]
        table_ref, anom_ref, out_ref, carry_ref = refs[5:9]
        incr_ref, index_ref, weight_ref, acc_ref, anom_sem, incr_sem, some_sem = refs[9:]
    else:
        info_ref, anom_hbm, incr_hbm, index_hbm, weight_hbm, tiles_hbm, carry_ref = refs[:7]
        table_ref, anom_ref, out_ref, tiles_ref = refs[9:13]
        incr_ref, index_ref, weight_ref, acc_ref, anom_sem, incr_sem, some_sem = refs[13:]
    flip = info_ref[0] == 1
    low = jnp.where(flip, chunks - done - steps, done)

    def chunk_of(i):
        return jnp.where(flip, chunks - 1 - done - i, done + i)

    def lanes(c, count=1):
        return pl.ds(pl.multiple_of(c * CHUNK, CHUNK), count * CHUNK)

    index_copy = pltpu.make_async_copy(index_hbm.at[:, lanes(low, steps)], index_ref, some_sem.at[0])
    weight_copy = pltpu.make_async_copy(
        weight_hbm.at[:, lanes(low, steps)], weight_ref, some_sem.at[1]
    )
    index_copy.start()
    weight_copy.start()

    def chunk_copies(i):
        c = chunk_of(i)
        return (
            pltpu.make_async_copy(anom_hbm.at[:, :, lanes(c)], anom_ref.at[c], anom_sem.at[i]),
            pltpu.make_async_copy(incr_hbm.at[:, lanes(c)], incr_ref.at[i], incr_sem.at[i]),
        )

    for i in range(steps):
        for copy in chunk_copies(i):
            copy.start()
    if first:
        acc_ref[...] = jnp.zeros(acc_ref.shape, F32)
    else:
        tiles_copy = pltpu.make_async_copy(tiles_hbm, tiles_ref, some_sem.at[2])
        tiles_copy.start()
        acc_ref[...] = carry_ref[...]
    index_copy.wait()
    weight_copy.wait()
    rows = anom_ref.shape[1] * anom_ref.shape[2]
    total = steps if first else steps + 2

    def group(g, carry):
        acc0, acc1 = acc_ref[0], acc_ref[1]
        steps_here = [g * unroll + j for j in range(unroll)]
        for i in steps_here:
            for copy in chunk_copies(i):
                copy.wait()
        for i in steps_here:
            c = chunk_of(i)
            here = lanes(c - low)
            build_table(index_ref[:, here] - c * BLOCK, weight_ref[:, here], table_ref.at[c])
            weighted = (anom_ref[c].astype(F32) * incr_ref[i][None]).astype(BF16)
            window = lax.dot_general(
                table_ref[c],
                weighted.reshape(rows, CHUNK),
                (((1,), (1,)), ((), ())),
                preferred_element_type=F32,
            )
            near, mid, far = window[:BLOCK], window[BLOCK : 2 * BLOCK], window[2 * BLOCK :]
            ready = acc0 + jnp.where(flip, far, near)
            out_ref[jnp.where(flip, total - 1 - i, i)] = ready.T.astype(BF16)
            acc0 = acc1 + mid
            acc1 = jnp.where(flip, near, far)
        acc_ref[0] = acc0
        acc_ref[1] = acc1
        return carry

    lax.fori_loop(0, steps // unroll, group, 0)
    if first:
        carry_ref[...] = acc_ref[...]
    else:
        out_ref[jnp.where(flip, 1, steps)] = acc_ref[0].T.astype(BF16)
        out_ref[jnp.where(flip, 0, steps + 1)] = acc_ref[1].T.astype(BF16)
        tiles_copy.wait()


def spread_call(steps, done, unroll, info, anomalies, increment, index, weight, extra=()):
    members, fields, columns = anomalies.shape
    rows = members * fields
    chunks = columns // CHUNK
    first = done == 0
    in_specs = [IN_SMEM, ANY, ANY, ANY, ANY]
    out_shape = [
        VMEM((chunks, WIN, CHUNK), BF16),
        VMEM((chunks, members, fields, CHUNK), BF16),
        jax.ShapeDtypeStruct((chunks // 2 + 1, rows, BLOCK), BF16),
    ]
    aliases = {}
    if first:
        out_shape.append(VMEM((2, BLOCK, rows), F32))
    else:
        in_specs += [ANY, IN_VMEM, IN_VMEM, IN_VMEM]
        out_shape.append(VMEM(extra[0].shape, BF16))
        aliases = {7: 0, 8: 1}
    return call(
        functools.partial(spread_kernel, steps, done, unroll, chunks),
        in_specs,
        [IN_VMEM] * 4,
        out_shape,
        [
            VMEM((steps, fields, CHUNK), F32),
            VMEM((INTP, steps * CHUNK), jnp.int32),
            VMEM((INTP, steps * CHUNK), F32),
            VMEM((2, BLOCK, rows), F32),
            pltpu.SemaphoreType.DMA((steps,)),
            pltpu.SemaphoreType.DMA((steps,)),
            pltpu.SemaphoreType.DMA((3,)),
        ],
        aliases,
    )(info, in_hbm(anomalies), in_hbm(increment), in_hbm(index), in_hbm(weight), *extra)


def convolve(wide_ref, tiles_ref, nbr_ref, smooth_ref, b):
    count = tiles_ref.shape[1]
    picked = jnp.concatenate([wide_ref[nbr_ref[n, b]] for n in range(count)], axis=1)
    weights = tiles_ref[b].reshape(count * BLOCK, BLOCK)
    smooth = jnp.dot(picked, weights, preferred_element_type=F32)
    smooth_ref[b + 1] = smooth.astype(BF16)


def conv_early_kernel(
    unroll, info_ref, nbr_ref, own_a, own_b, got_a, tiles_ref, wide_ref, smooth_ref, edge_ref
):
    half = own_a.shape[0]
    reach = half - 1
    blocks = tiles_ref.shape[0]
    top = blocks + reach
    flip = info_ref[0] == 1

    @pl.when(jnp.logical_not(flip))
    def _():
        wide_ref[reach - 1 : reach - 1 + half] = own_b[...]
        wide_ref[reach - 1 + half : top - 1] = own_a[0 : half - 2]
        wide_ref[top - 1 : top + 1] = (
            got_a[0:2].astype(F32) + own_a[half - 2 : half].astype(F32)
        ).astype(BF16)
        wide_ref[top + 1 : top + reach] = got_a[2:half]

    @pl.when(flip)
    def _():
        wide_ref[0 : reach - 1] = got_a[0 : reach - 1]
        wide_ref[reach - 1 : reach + 1] = (
            got_a[reach - 1 : reach + 1].astype(F32) + own_a[0:2].astype(F32)
        ).astype(BF16)
        wide_ref[reach + 1 : reach - 1 + half] = own_a[2:half]
        wide_ref[reach - 1 + half : top + 1] = own_b[...]

    early = blocks - half
    start = jnp.where(flip, 0, half)
    groups(
        early, unroll, lambda i: convolve(wide_ref, tiles_ref, nbr_ref, smooth_ref, start + i)
    )
    edge_ref[...] = smooth_ref[jnp.where(flip, 1, blocks)]


def conv_late_kernel(
    unroll, info_ref, nbr_ref, got_b, tiles_ref, wide_in, smooth_in, wide_ref, smooth_ref, edge_ref
):
    half = got_b.shape[0]
    reach = half - 1
    blocks = tiles_ref.shape[0]
    top = blocks + reach
    flip = info_ref[0] == 1
    present = info_ref[1] == 1
    beyond = jnp.where(present, got_b[...], jnp.zeros(got_b.shape, BF16))

    @pl.when(jnp.logical_not(flip))
    def _():
        wide_ref[0 : reach - 1] = beyond[0 : reach - 1]
        both = wide_ref[reach - 1 : reach + 1].astype(F32) + beyond[reach - 1 :].astype(F32)
        wide_ref[reach - 1] = jnp.where(present, both[0], jnp.zeros_like(both[0])).astype(BF16)
        wide_ref[reach] = both[1].astype(BF16)

    @pl.when(flip)
    def _():
        wide_ref[top + 1 : top + reach] = beyond[2:half]
        both = wide_ref[top - 1 : top + 1].astype(F32) + beyond[0:2].astype(F32)
        wide_ref[top - 1] = both[0].astype(BF16)
        wide_ref[top] = jnp.where(present, both[1], jnp.zeros_like(both[1])).astype(BF16)

    start = jnp.where(flip, blocks - half, 0)
    groups(half, unroll, lambda i: convolve(wide_ref, tiles_ref, nbr_ref, smooth_ref, start + i))
    edge_ref[...] = smooth_ref[jnp.where(flip, blocks, 1)]


def conv_early_call(info, neighbours, own_a, own_b, got_a, tiles):
    blocks, _ = tiles.shape[:2]
    half, rows, _ = own_a.shape
    early = blocks - half
    return call(
        functools.partial(conv_early_kernel, early),
        [IN_SMEM, IN_SMEM] + [IN_VMEM] * 4,
        [IN_VMEM] * 3,
        [
            VMEM((blocks + 2 * half - 2, rows, BLOCK), BF16),
            VMEM((blocks + 2, rows, BLOCK), BF16),
            jax.ShapeDtypeStruct((rows, BLOCK), BF16),
        ],
        [],
    )(info, neighbours, own_a, own_b, got_a, tiles)


def conv_late_call(info, neighbours, got_b, tiles, wide, smooth):
    _, rows, _ = got_b.shape
    return call(
        functools.partial(conv_late_kernel, 3),
        [IN_SMEM, IN_SMEM] + [IN_VMEM] * 4,
        [IN_VMEM] * 3,
        [
            VMEM(wide.shape, BF16),
            VMEM(smooth.shape, BF16),
            jax.ShapeDtypeStruct((rows, BLOCK), BF16),
        ],
        [],
        {4: 0, 5: 1},
    )(info, neighbours, got_b, tiles, wide, smooth)


def back_kernel(part, steps, unroll, per, *refs):
    if part == 0:
        info_ref, got_ref, table_ref, anom_ref, _, smooth_ref, out_ref = refs
    elif part == 1:
        info_ref, table_ref, anom_ref, smooth_ref, _, out_ref = refs
    else:
        info_ref, got_ref, table_ref, anom_ref, _, _, smooth_ref, out_ref = refs
    flip = info_ref[0] == 1
    blocks = table_ref.shape[0]
    shares = out_ref.shape[0]
    if part == 0:
        smooth_ref[jnp.where(flip, 0, blocks + 1)] = got_ref[...]
        start = jnp.where(flip, 0, blocks - steps)
    elif part == 1:
        start = jnp.where(flip, blocks - 1 - steps, 1)
    else:
        got = got_ref[...]
        present = info_ref[1] == 1
        smooth_ref[jnp.where(flip, blocks + 1, 0)] = jnp.where(present, got, jnp.zeros_like(got))
        start = jnp.where(flip, blocks - 1, 0)

    def body(i):
        c = start + i
        lhs = jnp.concatenate([smooth_ref[c], smooth_ref[c + 1], smooth_ref[c + 2]], axis=1)
        returned = jnp.dot(lhs, table_ref[c], preferred_element_type=F32)
        anom = anom_ref[c].astype(F32)
        value = jnp.sum(anom * returned.reshape(anom.shape), axis=0)
        lane = pl.multiple_of(lax.rem(c, per) * CHUNK, CHUNK)
        place = lax.div(c, per) - info_ref[2]
        place = jnp.where(place < 0, place + shares, place)
        out_ref[place, :, pl.ds(lane, CHUNK)] = value.astype(BF16)

    groups(steps, unroll, body)


def back_call(part, steps, unroll, shares, info, got, table, anom, smooth, out=None):
    chunks, _, fields, _ = anom.shape
    per = chunks // shares
    operands = [info] + ([] if part == 1 else [got]) + [table, anom, smooth]
    in_specs = [IN_SMEM] + [IN_VMEM] * (len(operands) - 1)
    out_type = VMEM((shares, fields, per * CHUNK), BF16)
    if part == 2:
        out_type = jax.ShapeDtypeStruct(out_type.shape, BF16)
    smooth_type = VMEM(smooth.shape, BF16)
    last = len(operands) - 1
    if part == 0:
        out_shape, aliases = [smooth_type, out_type], {last: 0}
    elif part == 1:
        operands, in_specs = operands + [out], in_specs + [IN_VMEM]
        out_shape, aliases = [out_type], {last + 1: 0}
    else:
        operands, in_specs = operands + [out], in_specs + [IN_VMEM]
        out_shape, aliases = [smooth_type, out_type], {last: 0, last + 1: 1}
    return call(
        functools.partial(back_kernel, part, steps, unroll, per),
        in_specs,
        [IN_VMEM] * len(out_shape),
        out_shape,
        [],
        aliases,
    )(*operands)


def swaps(count):
    inner = [(i, i ^ 1) for i in range(count)]
    outer = [(i, (i + 1) % count if i % 2 else (i - 1) % count) for i in range(count)]
    return inner, outer


def swap(value, pairs):
    return lax.ppermute(value, "space", pairs)


def shards(increment, anomalies, interp_index, interp_weight, neighbour_blocks, tiles):
    members, _, columns = anomalies.shape
    chunks = columns // CHUNK
    space = lax.axis_index("space")
    count = lax.axis_size("space")
    mem = lax.axis_index("mem")
    shares = lax.axis_size("mem")
    assert count % 2 == 0
    flip = space & 1
    inner, outer = swaps(count)
    head = chunks // 2 + 1
    present = jnp.where(flip == 1, space < count - 1, space > 0)
    info = jnp.stack([flip, present.astype(jnp.int32), mem]).astype(jnp.int32)
    columns_in = (anomalies, increment, interp_index, interp_weight)
    table, anom, own_b, carry = spread_call(head, 0, 3, info, *columns_in)
    got_b = swap(own_b, outer)
    table, anom, own_a, tiles_here = spread_call(
        chunks - head, head, 1, info, *columns_in, (in_hbm(tiles), carry, table, anom)
    )
    got_a = swap(own_a, inner)
    wide, smooth, edge_a = conv_early_call(info, neighbour_blocks, own_a, own_b, got_a, tiles_here)
    halo_a = swap(edge_a, inner)
    smooth, out = back_call(0, chunks - head - 1, 3, shares, info, halo_a, table, anom, smooth)
    wide, smooth, edge_b = conv_late_call(info, neighbour_blocks, got_b, tiles_here, wide, smooth)
    halo_b = swap(edge_b, outer)
    (out,) = back_call(1, head, 3, shares, info, None, table, anom, smooth, out)
    _, pieces = back_call(2, 1, 1, shares, info, halo_b, table, anom, smooth, out)

    total = pieces[0].astype(F32)
    for shift in range(1, shares):
        got = lax.ppermute(
            pieces[shift],
            "mem",
            [(i, (i + shift) % shares) for i in range(shares)],
        )
        total = total + got.astype(F32)
    return total / (members * shares - 1)


def solution(mesh):
    in_specs = (
        P(None, "space"),
        P("mem", None, "space"),
        P(None, "space"),
        P(None, "space"),
        P(None, "space"),
        P("space", None, None, None),
    )
    out_specs = P(None, ("space", "mem"))
    return jax.shard_map(shards, mesh=mesh, in_specs=in_specs, out_specs=out_specs, check_vma=False)
```

```python
import functools

import jax
import jax.numpy as jnp
from jax import lax
from jax.experimental import pallas as pl
from jax.experimental.pallas import tpu as pltpu
from jax.sharding import PartitionSpec as P


BLOCK = 128
HI = 128
RATIO = 4
CHUNK = RATIO * BLOCK
WIN = 3 * BLOCK
REACH = 2 * HI + 32
F32 = jnp.float32
BF16 = jnp.bfloat16
FIRST_UNROLL = 9
REST_UNROLL = 7
VMEM = pltpu.VMEM
ANY = pl.BlockSpec(memory_space=pl.ANY)
IN_VMEM = pl.BlockSpec(memory_space=pltpu.VMEM)
IN_SMEM = pl.BlockSpec(memory_space=pltpu.SMEM)


def is_present():
    space = lax.axis_index("space")
    last = lax.axis_size("space") - 1
    return jnp.where((space & 1) == 1, space < last, space > 0)


def in_hbm(x):
    return pltpu.with_memory_space_constraint(x, pltpu.HBM)


def call(kernel, in_specs, out_specs, out_shape, scratch, aliases=None):
    return pl.pallas_call(
        kernel,
        in_specs=in_specs,
        out_specs=out_specs,
        out_shape=out_shape,
        scratch_shapes=scratch,
        input_output_aliases=aliases or {},
        compiler_params=pltpu.CompilerParams(vmem_limit_bytes=16 * 1024 * 1024),
        cost_estimate=pl.CostEstimate(flops=0, bytes_accessed=0, transcendentals=0),
    )


def groups(steps, unroll, body):
    unroll = unroll if steps % unroll == 0 else 1

    def group(g, carry):
        for j in range(unroll):
            body(g * unroll + j)
        return carry

    lax.fori_loop(0, steps // unroll, group, 0)


def build_table(local, weight):
    i0, i1, i2 = local[0:1], local[1:2], local[2:3]
    w0, w1, w2 = weight[0:1], weight[1:2], weight[2:3]
    zero = jnp.zeros_like(w0)
    w0 = w0 + jnp.where(i1 == i0, w1, zero) + jnp.where(i2 == i0, w2, zero)
    w1 = w1 + jnp.where(i2 == i1, w2, zero)
    rows = REACH // 16
    iota = lax.broadcasted_iota(jnp.int32, (rows, 16, BLOCK), 0) * 16 + lax.broadcasted_iota(
        jnp.int32, (rows, 16, BLOCK), 1
    )
    iota = iota.astype(jnp.int16)
    parts = []
    for s in range(CHUNK // BLOCK):
        cols = slice(s * BLOCK, (s + 1) * BLOCK)
        base = s * BLOCK // RATIO

        def wide(x, kind):
            return jnp.broadcast_to(x[:, cols], (16, BLOCK)).astype(kind)[None]

        table = jnp.zeros((1, 16, BLOCK), BF16)
        for index, value in ((i2, w2), (i1, w1), (i0, w0)):
            table = jnp.where(wide(index - base, jnp.int16) == iota, wide(value, BF16), table)
        pieces = [table.reshape(REACH, BLOCK)]
        if base:
            pieces.insert(0, jnp.zeros((base, BLOCK), BF16))
        if base + REACH < WIN:
            pieces.append(jnp.zeros((WIN - base - REACH, BLOCK), BF16))
        parts.append(jnp.concatenate(pieces, axis=0))
    return jnp.concatenate(parts, axis=1)


def is_flipped():
    return (lax.axis_index("space") & 1) == 1


def spread_kernel(steps, done, unroll, chunks, *refs):
    first = done == 0
    if first:
        anom_hbm, incr_hbm, index_hbm, weight_hbm, nbr_hbm = refs[:5]
        table_ref, out_ref, carry_ref = refs[5:8]
        anom_ref, incr_ref, index_ref, weight_ref, nbr_ref = refs[8:13]
        acc_ref, anom_sem, incr_sem, some_sem = refs[13:]
    else:
        anom_ref, incr_ref, index_ref, weight_ref, tiles_hbm, carry_ref = refs[:6]
        table_ref, out_ref, tiles_ref, acc_ref, tiles_sem = refs[7:]
        tiles_copy = pltpu.make_async_copy(tiles_hbm, tiles_ref, tiles_sem)
        tiles_copy.start()
    flip = is_flipped()

    def chunk_of(step):
        return jnp.where(flip, chunks - 1 - step, step)

    def lanes(c):
        return pl.ds(pl.multiple_of(c * CHUNK, CHUNK), CHUNK)

    def chunk_copies(step):
        c = chunk_of(step)
        return (
            pltpu.make_async_copy(anom_hbm.at[:, :, lanes(c)], anom_ref.at[c], anom_sem.at[step]),
            pltpu.make_async_copy(incr_hbm.at[:, lanes(c)], incr_ref.at[c], incr_sem.at[step]),
        )

    if first:
        copies = [
            pltpu.make_async_copy(source, target, some_sem.at[k])
            for k, (source, target) in enumerate(
                (
                    (index_hbm, index_ref),
                    (weight_hbm, weight_ref),
                    (nbr_hbm, nbr_ref),
                )
            )
        ]
        for copy in copies[:2]:
            copy.start()
        for step in range(chunks):
            for copy in chunk_copies(step):
                copy.start()
        for copy in copies[2:]:
            copy.start()
        acc_ref[...] = jnp.zeros(acc_ref.shape, F32)
        for copy in copies[:2]:
            copy.wait()
    else:
        acc_ref[...] = carry_ref[...]
    rows = anom_ref.shape[1] * anom_ref.shape[2]
    total = steps if first else steps + 2

    def group(g, carry):
        acc0, acc1 = acc_ref[0], acc_ref[1]
        here = [g * unroll + j for j in range(unroll)]
        if first:
            for i in here:
                for copy in chunk_copies(i):
                    copy.wait()
        for i in here:
            c = chunk_of(done + i)
            table = build_table(index_ref[:, lanes(c)] - c * BLOCK, weight_ref[:, lanes(c)])
            table_ref[c] = table
            weighted = (anom_ref[c].astype(F32) * incr_ref[c][None]).astype(BF16)
            window = lax.dot_general(
                table,
                weighted.reshape(rows, CHUNK),
                (((1,), (1,)), ((), ())),
                preferred_element_type=F32,
            )
            near, mid, far = window[:BLOCK], window[BLOCK : 2 * BLOCK], window[2 * BLOCK :]
            ready = acc0 + jnp.where(flip, far, near)
            out_ref[jnp.where(flip, total - 1 - i, i)] = ready.T.astype(BF16)
            acc0 = acc1 + mid
            acc1 = jnp.where(flip, near, far)
        acc_ref[0] = acc0
        acc_ref[1] = acc1
        return carry

    lax.fori_loop(0, steps // unroll, group, 0)
    if first:
        carry_ref[...] = acc_ref[...]
        for step in range(steps, chunks):
            for copy in chunk_copies(step):
                copy.wait()
        for copy in copies[2:]:
            copy.wait()
    else:
        out_ref[jnp.where(flip, 1, steps)] = acc_ref[0].T.astype(BF16)
        out_ref[jnp.where(flip, 0, steps + 1)] = acc_ref[1].T.astype(BF16)
        tiles_copy.wait()


def spread_first_call(steps, unroll, increment, anomalies, index, weight, neighbours):
    members, fields, columns = anomalies.shape
    rows = members * fields
    chunks = columns // CHUNK
    return call(
        functools.partial(spread_kernel, steps, 0, unroll, chunks),
        [ANY] * 5,
        [IN_VMEM] * 7 + [IN_SMEM],
        [
            VMEM((chunks, WIN, CHUNK), BF16),
            jax.ShapeDtypeStruct((steps, rows, BLOCK), BF16),
            VMEM((2, BLOCK, rows), F32),
            VMEM((chunks, members, fields, CHUNK), BF16),
            VMEM((chunks, fields, CHUNK), F32),
            VMEM(index.shape, jnp.int32),
            VMEM(weight.shape, F32),
            pltpu.SMEM(neighbours.shape, jnp.int32),
        ],
        [
            VMEM((2, BLOCK, rows), F32),
            pltpu.SemaphoreType.DMA((chunks,)),
            pltpu.SemaphoreType.DMA((chunks,)),
            pltpu.SemaphoreType.DMA((3,)),
        ],
    )(*(in_hbm(x) for x in (anomalies, increment, index, weight, neighbours)))


def spread_rest_call(steps, unroll, table, carry, columns, tiles):
    chunks = table.shape[0]
    rows = carry.shape[2]
    return call(
        functools.partial(spread_kernel, steps, chunks - steps, unroll, chunks),
        [IN_VMEM] * 4 + [ANY] + [IN_VMEM] * 2,
        [IN_VMEM] * 3,
        [
            VMEM(table.shape, BF16),
            jax.ShapeDtypeStruct((steps + 2, rows, BLOCK), BF16),
            VMEM(tiles.shape, BF16),
        ],
        [VMEM((2, BLOCK, rows), F32), pltpu.SemaphoreType.DMA(())],
        {6: 0},
    )(*columns, in_hbm(tiles), carry, table)


def convolve(wide_ref, tiles_ref, nbr_ref, b):
    count = tiles_ref.shape[1]
    picked = jnp.concatenate([wide_ref[nbr_ref[n, b]] for n in range(count)], axis=1)
    weights = tiles_ref[b].reshape(count * BLOCK, BLOCK)
    return jnp.dot(picked, weights, preferred_element_type=F32).astype(BF16)


def edge_early_kernel(nbr_ref, own_a, own_b, got_a, tiles_ref, wide_ref, smooth_ref, edge_ref):
    half = own_a.shape[0]
    reach = half - 1
    blocks = tiles_ref.shape[0]
    top = blocks + reach
    flip = is_flipped()

    @pl.when(jnp.logical_not(flip))
    def _():
        wide_ref[reach - 1 : reach - 1 + half] = own_b[...]
        wide_ref[reach - 1 + half : top - 1] = own_a[0 : half - 2]
        wide_ref[top - 1 : top + 1] = (
            got_a[0:2].astype(F32) + own_a[half - 2 : half].astype(F32)
        ).astype(BF16)
        wide_ref[top + 1 : top + reach] = got_a[2:half]

    @pl.when(flip)
    def _():
        wide_ref[0 : reach - 1] = got_a[0 : reach - 1]
        wide_ref[reach - 1 : reach + 1] = (
            got_a[reach - 1 : reach + 1].astype(F32) + own_a[0:2].astype(F32)
        ).astype(BF16)
        wide_ref[reach + 1 : reach - 1 + half] = own_a[2:half]
        wide_ref[reach - 1 + half : top + 1] = own_b[...]

    b = jnp.where(flip, 0, blocks - 1)
    edge = convolve(wide_ref, tiles_ref, nbr_ref, b)
    smooth_ref[b + 1] = edge
    edge_ref[...] = edge


def edge_late_kernel(
    nbr_ref, got_b, tiles_ref, wide_in, smooth_in, wide_ref, smooth_ref, edge_ref
):
    half = got_b.shape[0]
    reach = half - 1
    blocks = tiles_ref.shape[0]
    top = blocks + reach
    flip = is_flipped()
    present = is_present()
    beyond = jnp.where(present, got_b[...], jnp.zeros(got_b.shape, BF16))

    @pl.when(jnp.logical_not(flip))
    def _():
        wide_ref[0 : reach - 1] = beyond[0 : reach - 1]
        both = wide_ref[reach - 1 : reach + 1].astype(F32) + beyond[reach - 1 :].astype(F32)
        wide_ref[reach - 1] = jnp.where(present, both[0], jnp.zeros_like(both[0])).astype(BF16)
        wide_ref[reach] = both[1].astype(BF16)

    @pl.when(flip)
    def _():
        wide_ref[top + 1 : top + reach] = beyond[2:half]
        both = wide_ref[top - 1 : top + 1].astype(F32) + beyond[0:2].astype(F32)
        wide_ref[top - 1] = both[0].astype(BF16)
        wide_ref[top] = jnp.where(present, both[1], jnp.zeros_like(both[1])).astype(BF16)

    b = jnp.where(flip, blocks - 1, 0)
    edge = convolve(wide_ref, tiles_ref, nbr_ref, b)
    smooth_ref[b + 1] = edge
    edge_ref[...] = edge


def rest_kernel(early, steps, unroll, nbr_ref, wide_ref, tiles_ref, smooth_in, smooth_ref):
    blocks = tiles_ref.shape[0]
    flip = is_flipped()
    if early:
        start = jnp.where(flip, 1, blocks - 1 - steps)
    else:
        start = jnp.where(flip, blocks - 1 - steps, 1)

    def body(i):
        b = start + i
        smooth_ref[b + 1] = convolve(wide_ref, tiles_ref, nbr_ref, b)

    groups(steps, unroll, body)


def edge_early_call(neighbours, own_a, own_b, got_a, tiles):
    blocks = tiles.shape[0]
    half, rows, _ = own_a.shape
    return call(
        edge_early_kernel,
        [IN_SMEM] + [IN_VMEM] * 4,
        [IN_VMEM] * 3,
        [
            VMEM((blocks + 2 * half - 2, rows, BLOCK), BF16),
            VMEM((blocks + 2, rows, BLOCK), BF16),
            jax.ShapeDtypeStruct((rows, BLOCK), BF16),
        ],
        [],
    )(neighbours, own_a, own_b, got_a, tiles)


def edge_late_call(neighbours, got_b, tiles, wide, smooth):
    _, rows, _ = got_b.shape
    return call(
        edge_late_kernel,
        [IN_SMEM] + [IN_VMEM] * 4,
        [IN_VMEM] * 3,
        [
            VMEM(wide.shape, BF16),
            VMEM(smooth.shape, BF16),
            jax.ShapeDtypeStruct((rows, BLOCK), BF16),
        ],
        [],
        {3: 0, 4: 1},
    )(neighbours, got_b, tiles, wide, smooth)


def rest_call(early, steps, unroll, neighbours, wide, tiles, smooth):
    return call(
        functools.partial(rest_kernel, early, steps, unroll),
        [IN_SMEM] + [IN_VMEM] * 3,
        [IN_VMEM],
        [VMEM(smooth.shape, BF16)],
        [],
        {3: 0},
    )(neighbours, wide, tiles, smooth)[0]


def back_kernel(part, steps, unroll, per, *refs):
    if part == 0:
        got_ref, table_ref, anom_ref, _, smooth_ref, out_ref = refs
    elif part == 1:
        table_ref, anom_ref, smooth_ref, _, out_ref = refs
    else:
        got_ref, table_ref, anom_ref, _, _, smooth_ref, out_ref = refs
    flip = is_flipped()
    blocks = table_ref.shape[0]
    shares = out_ref.shape[0]
    if part == 0:
        smooth_ref[jnp.where(flip, 0, blocks + 1)] = got_ref[...]
        start = jnp.where(flip, 0, blocks - steps)
    elif part == 1:
        start = jnp.where(flip, blocks - 1 - steps, 1)
    else:
        got = got_ref[...]
        present = is_present()
        smooth_ref[jnp.where(flip, blocks + 1, 0)] = jnp.where(present, got, jnp.zeros_like(got))
        start = jnp.where(flip, blocks - 1, 0)

    def body(i):
        c = start + i
        lhs = jnp.concatenate([smooth_ref[c], smooth_ref[c + 1], smooth_ref[c + 2]], axis=1)
        returned = jnp.dot(lhs, table_ref[c], preferred_element_type=F32)
        anom = anom_ref[c].astype(F32)
        value = jnp.sum(anom * returned.reshape(anom.shape), axis=0)
        lane = pl.multiple_of(lax.rem(c, per) * CHUNK, CHUNK)
        place = lax.div(c, per) - lax.axis_index("mem")
        place = jnp.where(place < 0, place + shares, place)
        out_ref[place, :, pl.ds(lane, CHUNK)] = value.astype(BF16)

    groups(steps, unroll, body)


def back_call(part, steps, unroll, shares, got, table, anom, smooth, out=None):
    chunks, _, fields, _ = anom.shape
    per = chunks // shares
    operands = ([] if part == 1 else [got]) + [table, anom, smooth]
    in_specs = [IN_VMEM] * len(operands)
    out_type = VMEM((shares, fields, per * CHUNK), BF16)
    if part == 2:
        out_type = jax.ShapeDtypeStruct(out_type.shape, BF16)
    smooth_type = VMEM(smooth.shape, BF16)
    last = len(operands) - 1
    if part == 0:
        out_shape, aliases = [smooth_type, out_type], {last: 0}
    elif part == 1:
        operands, in_specs = operands + [out], in_specs + [IN_VMEM]
        out_shape, aliases = [out_type], {last + 1: 0}
    else:
        operands, in_specs = operands + [out], in_specs + [IN_VMEM]
        out_shape, aliases = [smooth_type, out_type], {last: 0, last + 1: 1}
    return call(
        functools.partial(back_kernel, part, steps, unroll, per),
        in_specs,
        [IN_VMEM] * len(out_shape),
        out_shape,
        [],
        aliases,
    )(*operands)


def swaps(count, shares):
    inner, outer = [], []
    for i in range(count):
        far = i + 1 if i % 2 else i - 1
        for m in range(shares):
            here = i * shares + m
            inner.append((here, (i ^ 1) * shares + m))
            outer.append((here, far * shares + m if 0 <= far < count else i * shares + (m ^ 1)))
    return inner, outer


def swap(value, pairs):
    return lax.ppermute(value, ("space", "mem"), pairs)


def shards(increment, anomalies, interp_index, interp_weight, neighbour_blocks, tiles):
    members, _, columns = anomalies.shape
    chunks = columns // CHUNK
    count = lax.axis_size("space")
    shares = lax.axis_size("mem")
    assert count % 2 == 0 and shares % 2 == 0
    inner, outer = swaps(count, shares)
    head = chunks // 2 + 1
    table, own_b, carry, anom, *columns_here, neighbours = spread_first_call(
        head,
        FIRST_UNROLL,
        increment,
        anomalies,
        interp_index,
        interp_weight,
        neighbour_blocks,
    )
    got_b = swap(own_b, outer)
    table, own_a, tiles = spread_rest_call(
        chunks - head, REST_UNROLL, table, carry, (anom, *columns_here), tiles
    )
    got_a = swap(own_a, inner)
    early = chunks - head - 1
    wide, smooth, edge_a = edge_early_call(neighbours, own_a, own_b, got_a, tiles)
    halo_a = swap(edge_a, inner)
    smooth = rest_call(True, early, 3, neighbours, wide, tiles, smooth)
    smooth, out = back_call(0, early, 3, shares, halo_a, table, anom, smooth)
    wide, smooth, edge_b = edge_late_call(neighbours, got_b, tiles, wide, smooth)
    halo_b = swap(edge_b, outer)
    smooth = rest_call(False, head - 1, 4, neighbours, wide, tiles, smooth)
    (out,) = back_call(1, head, 3, shares, None, table, anom, smooth, out)
    _, pieces = back_call(2, 1, 1, shares, halo_b, table, anom, smooth, out)
    total = pieces[0].astype(F32)
    for shift in range(1, shares):
        got = lax.ppermute(
            pieces[shift],
            "mem",
            [(i, (i + shift) % shares) for i in range(shares)],
        )
        total = total + got.astype(F32)
    return total / (members * shares - 1)


def solution(mesh):
    in_specs = (
        P(None, "space"),
        P("mem", None, "space"),
        P(None, "space"),
        P(None, "space"),
        P(None, "space"),
        P("space", None, None, None),
    )
    out_specs = P(None, ("space", "mem"))
    return jax.shard_map(shards, mesh=mesh, in_specs=in_specs, out_specs=out_specs, check_vma=False)
```

```python
import functools

import jax
import jax.numpy as jnp
from jax import lax
from jax.experimental import pallas as pl
from jax.experimental.pallas import tpu as pltpu
from jax.sharding import PartitionSpec as P


BLOCK = 128
HI = 128
RATIO = 4
CHUNK = RATIO * BLOCK
WIN = 3 * BLOCK
REACH = 2 * HI + 32
F32 = jnp.float32
BF16 = jnp.bfloat16
NEAR = 5
VMEM = pltpu.VMEM
ANY = pl.BlockSpec(memory_space=pl.ANY)
IN_VMEM = pl.BlockSpec(memory_space=pltpu.VMEM)
IN_SMEM = pl.BlockSpec(memory_space=pltpu.SMEM)


def is_present():
    space = lax.axis_index("space")
    last = lax.axis_size("space") - 1
    return jnp.where((space & 1) == 1, space < last, space > 0)


def in_hbm(x):
    return pltpu.with_memory_space_constraint(x, pltpu.HBM)


def call(kernel, in_specs, out_specs, out_shape, scratch, aliases=None):
    return pl.pallas_call(
        kernel,
        in_specs=in_specs,
        out_specs=out_specs,
        out_shape=out_shape,
        scratch_shapes=scratch,
        input_output_aliases=aliases or {},
        compiler_params=pltpu.CompilerParams(vmem_limit_bytes=16 * 1024 * 1024),
        cost_estimate=pl.CostEstimate(flops=0, bytes_accessed=0, transcendentals=0),
    )


def groups(steps, unroll, body):
    unroll = unroll if steps % unroll == 0 else 1

    def group(g, carry):
        for j in range(unroll):
            body(g * unroll + j)
        return carry

    lax.fori_loop(0, steps // unroll, group, 0)


def build_table(local, weight):
    i0, i1, i2 = local[0:1], local[1:2], local[2:3]
    w0, w1, w2 = weight[0:1], weight[1:2], weight[2:3]
    zero = jnp.zeros_like(w0)
    w0 = w0 + jnp.where(i1 == i0, w1, zero) + jnp.where(i2 == i0, w2, zero)
    w1 = w1 + jnp.where(i2 == i1, w2, zero)
    rows = REACH // 16
    iota = lax.broadcasted_iota(jnp.int32, (rows, 16, BLOCK), 0) * 16 + lax.broadcasted_iota(
        jnp.int32, (rows, 16, BLOCK), 1
    )
    iota = iota.astype(jnp.int16)
    parts = []
    for s in range(CHUNK // BLOCK):
        cols = slice(s * BLOCK, (s + 1) * BLOCK)
        base = s * BLOCK // RATIO

        def wide(x, kind):
            return jnp.broadcast_to(x[:, cols], (16, BLOCK)).astype(kind)[None]

        table = jnp.zeros((1, 16, BLOCK), BF16)
        for index, value in ((i2, w2), (i1, w1), (i0, w0)):
            table = jnp.where(wide(index - base, jnp.int16) == iota, wide(value, BF16), table)
        pieces = [table.reshape(REACH, BLOCK)]
        if base:
            pieces.insert(0, jnp.zeros((base, BLOCK), BF16))
        if base + REACH < WIN:
            pieces.append(jnp.zeros((WIN - base - REACH, BLOCK), BF16))
        parts.append(jnp.concatenate(pieces, axis=0))
    return jnp.concatenate(parts, axis=1)


def is_flipped():
    return (lax.axis_index("space") & 1) == 1


def spread_kernel(steps, done, chunks, *refs):
    first, last = done == 0, done + steps == chunks
    if first:
        anom_hbm, incr_hbm, index_hbm, weight_hbm, nbr_hbm = refs[:5]
        table_ref, out_ref, carry_ref = refs[5:8]
        anom_ref, incr_ref, index_ref, weight_ref, nbr_ref = refs[8:13]
        anom_sem, incr_sem, some_sem = refs[13:]
    else:
        anom_ref, incr_ref, index_ref, weight_ref, carry_in = refs[:5]
        table_ref, out_ref = refs[6:8]
        carry_ref = refs[-1]
    flip = is_flipped()

    def chunk_of(step):
        return jnp.where(flip, chunks - 1 - step, step)

    def lanes(c):
        return pl.ds(pl.multiple_of(c * CHUNK, CHUNK), CHUNK)

    if first:
        copies = [
            pltpu.make_async_copy(source, target, some_sem.at[k])
            for k, (source, target) in enumerate(
                ((index_hbm, index_ref), (weight_hbm, weight_ref), (nbr_hbm, nbr_ref))
            )
        ]
        columns = []
        for k, (begin, end) in enumerate(((0, steps), (steps, chunks))):
            low = jnp.where(flip, chunks - end, begin)
            here = pl.ds(pl.multiple_of(low * CHUNK, CHUNK), (end - begin) * CHUNK)
            columns.append(
                (
                    pltpu.make_async_copy(
                        anom_hbm.at[:, :, here], anom_ref.at[:, :, here], anom_sem.at[k]
                    ),
                    pltpu.make_async_copy(
                        incr_hbm.at[:, here], incr_ref.at[:, here], incr_sem.at[k]
                    ),
                )
            )
        for copy in (*copies[:2], *columns[0], *columns[1], copies[2]):
            copy.start()
        acc0 = acc1 = jnp.zeros(carry_ref.shape[1:], F32)
        for copy in copies[:2]:
            copy.wait()
    else:
        acc0, acc1 = carry_in[0], carry_in[1]
    rows = anom_ref.shape[0] * anom_ref.shape[1]
    total = out_ref.shape[0]

    def table_of(i):
        c = chunk_of(done + i)
        table = build_table(index_ref[:, lanes(c)] - c * BLOCK, weight_ref[:, lanes(c)])
        table_ref[c] = table
        return table

    before = steps if first else 0
    if first:
        for i in range(before):
            table_of(i)
        for copy in columns[0]:
            copy.wait()
    for i in range(steps):
        c = chunk_of(done + i)
        table = table_ref[c] if i < before else table_of(i)
        weighted = (anom_ref[:, :, lanes(c)].astype(F32) * incr_ref[:, lanes(c)][None]).astype(BF16)
        window = lax.dot_general(
            table,
            weighted.reshape(rows, CHUNK),
            (((1,), (1,)), ((), ())),
            preferred_element_type=F32,
        )
        near, mid, far = window[:BLOCK], window[BLOCK : 2 * BLOCK], window[2 * BLOCK :]
        ready = acc0 + jnp.where(flip, far, near)
        out_ref[jnp.where(flip, total - 1 - i, i)] = ready.T.astype(BF16)
        acc0 = acc1 + mid
        acc1 = jnp.where(flip, near, far)
    if last:
        out_ref[jnp.where(flip, 1, steps)] = acc0.T.astype(BF16)
        out_ref[jnp.where(flip, 0, steps + 1)] = acc1.T.astype(BF16)
    else:
        carry_ref[0] = acc0
        carry_ref[1] = acc1
    if first:
        for copy in (*columns[1], copies[2]):
            copy.wait()


def spread_first_call(steps, increment, anomalies, index, weight, neighbours):
    members, fields, columns = anomalies.shape
    rows = members * fields
    chunks = columns // CHUNK
    return call(
        functools.partial(spread_kernel, steps, 0, chunks),
        [ANY] * 5,
        [IN_VMEM] * 7 + [IN_SMEM],
        [
            VMEM((chunks, WIN, CHUNK), BF16),
            jax.ShapeDtypeStruct((steps, rows, BLOCK), BF16),
            VMEM((2, BLOCK, rows), F32),
            VMEM(anomalies.shape, BF16),
            VMEM(increment.shape, F32),
            VMEM(index.shape, jnp.int32),
            VMEM(weight.shape, F32),
            pltpu.SMEM(neighbours.shape, jnp.int32),
        ],
        [
            pltpu.SemaphoreType.DMA((2,)),
            pltpu.SemaphoreType.DMA((2,)),
            pltpu.SemaphoreType.DMA((3,)),
        ],
    )(*(in_hbm(x) for x in (anomalies, increment, index, weight, neighbours)))


def spread_more_call(done, steps, table, carry, columns):
    chunks = table.shape[0]
    rows = carry.shape[2]
    last = done + steps == chunks
    out_shape = [
        VMEM(table.shape, BF16),
        jax.ShapeDtypeStruct((steps + 2 * last, rows, BLOCK), BF16),
    ]
    if not last:
        out_shape.append(VMEM(carry.shape, F32))
    return call(
        functools.partial(spread_kernel, steps, done, chunks),
        [IN_VMEM] * 6,
        [IN_VMEM] * len(out_shape),
        out_shape,
        [],
        {5: 0},
    )(*columns, carry, table)


def convolve(wide_ref, tiles_ref, nbr_ref, b):
    count = tiles_ref.shape[1]
    picked = jnp.concatenate([wide_ref[nbr_ref[n, b]] for n in range(count)], axis=1)
    weights = tiles_ref[b].reshape(count * BLOCK, BLOCK)
    return jnp.dot(picked, weights, preferred_element_type=F32).astype(BF16)


def edge_early_kernel(
    nbr_ref, own_a, own_near, own_far, got_a, tiles_ref, wide_ref, smooth_ref, edge_ref
):
    half = own_a.shape[0]
    near = own_near.shape[0]
    reach = half - 1
    blocks = tiles_ref.shape[0]
    top = blocks + reach
    flip = is_flipped()

    @pl.when(jnp.logical_not(flip))
    def _():
        wide_ref[reach - 1 : reach - 1 + near] = own_near[...]
        wide_ref[reach - 1 + near : reach - 1 + half] = own_far[...]
        wide_ref[reach - 1 + half : top - 1] = own_a[0 : half - 2]
        wide_ref[top - 1 : top + 1] = (
            got_a[0:2].astype(F32) + own_a[half - 2 : half].astype(F32)
        ).astype(BF16)
        wide_ref[top + 1 : top + reach] = got_a[2:half]

    @pl.when(flip)
    def _():
        wide_ref[0 : reach - 1] = got_a[0 : reach - 1]
        wide_ref[reach - 1 : reach + 1] = (
            got_a[reach - 1 : reach + 1].astype(F32) + own_a[0:2].astype(F32)
        ).astype(BF16)
        wide_ref[reach + 1 : reach - 1 + half] = own_a[2:half]
        wide_ref[reach - 1 + half : top + 1 - near] = own_far[...]
        wide_ref[top + 1 - near : top + 1] = own_near[...]

    b = jnp.where(flip, 0, blocks - 1)
    edge = convolve(wide_ref, tiles_ref, nbr_ref, b)
    smooth_ref[b + 1] = edge
    edge_ref[...] = edge


def edge_late_kernel(
    nbr_ref, got_near, got_far, tiles_ref, wide_in, smooth_in, wide_ref, smooth_ref, edge_ref
):
    near = got_near.shape[0]
    half = near + got_far.shape[0]
    reach = half - 1
    blocks = tiles_ref.shape[0]
    top = blocks + reach
    flip = is_flipped()
    present = is_present()

    def there(value):
        return jnp.where(present, value, jnp.zeros_like(value))

    @pl.when(jnp.logical_not(flip))
    def _():
        wide_ref[0 : half - near] = there(got_far[...])
        wide_ref[half - near : reach - 1] = there(got_near[0 : near - 2])
        both = wide_ref[reach - 1 : reach + 1].astype(F32) + there(got_near[near - 2 :].astype(F32))
        wide_ref[reach - 1] = there(both[0]).astype(BF16)
        wide_ref[reach] = both[1].astype(BF16)

    @pl.when(flip)
    def _():
        both = wide_ref[top - 1 : top + 1].astype(F32) + there(got_near[0:2].astype(F32))
        wide_ref[top - 1] = both[0].astype(BF16)
        wide_ref[top] = there(both[1]).astype(BF16)
        wide_ref[top + 1 : top - 1 + near] = there(got_near[2:near])
        wide_ref[top - 1 + near : top + reach] = there(got_far[...])

    b = jnp.where(flip, blocks - 1, 0)
    edge = convolve(wide_ref, tiles_ref, nbr_ref, b)
    smooth_ref[b + 1] = edge
    edge_ref[...] = edge


def rest_kernel(early, steps, unroll, nbr_ref, wide_ref, tiles_ref, smooth_in, smooth_ref):
    blocks = tiles_ref.shape[0]
    flip = is_flipped()
    if early:
        start = jnp.where(flip, 1, blocks - 1 - steps)
    else:
        start = jnp.where(flip, blocks - 1 - steps, 1)

    def body(i):
        b = start + i
        smooth_ref[b + 1] = convolve(wide_ref, tiles_ref, nbr_ref, b)

    groups(steps, unroll, body)


def edge_early_call(neighbours, own_a, own_near, own_far, got_a, tiles):
    blocks = tiles.shape[0]
    half, rows, _ = own_a.shape
    return call(
        edge_early_kernel,
        [IN_SMEM] + [IN_VMEM] * 5,
        [IN_VMEM] * 3,
        [
            VMEM((blocks + 2 * half - 2, rows, BLOCK), BF16),
            VMEM((blocks + 2, rows, BLOCK), BF16),
            jax.ShapeDtypeStruct((rows, BLOCK), BF16),
        ],
        [],
    )(neighbours, own_a, own_near, own_far, got_a, tiles)


def edge_late_call(neighbours, got_near, got_far, tiles, wide, smooth):
    _, rows, _ = got_near.shape
    return call(
        edge_late_kernel,
        [IN_SMEM] + [IN_VMEM] * 5,
        [IN_VMEM] * 3,
        [
            VMEM(wide.shape, BF16),
            VMEM(smooth.shape, BF16),
            jax.ShapeDtypeStruct((rows, BLOCK), BF16),
        ],
        [],
        {4: 0, 5: 1},
    )(neighbours, got_near, got_far, tiles, wide, smooth)


def rest_call(early, steps, unroll, neighbours, wide, tiles, smooth):
    return call(
        functools.partial(rest_kernel, early, steps, unroll),
        [IN_SMEM] + [IN_VMEM] * 3,
        [IN_VMEM],
        [VMEM(smooth.shape, BF16)],
        [],
        {3: 0},
    )(neighbours, wide, tiles, smooth)[0]


def back_kernel(part, steps, unroll, per, *refs):
    if part == 0:
        got_ref, table_ref, anom_ref, _, smooth_ref, out_ref = refs
    elif part == 1:
        table_ref, anom_ref, smooth_ref, _, out_ref = refs
    else:
        got_ref, table_ref, anom_ref, _, _, smooth_ref, out_ref = refs
    flip = is_flipped()
    blocks = table_ref.shape[0]
    shares = out_ref.shape[0]
    if part == 0:
        smooth_ref[jnp.where(flip, 0, blocks + 1)] = got_ref[...]
        start = jnp.where(flip, 0, blocks - steps)
    elif part == 1:
        start = jnp.where(flip, blocks - 1 - steps, 1)
    else:
        got = got_ref[...]
        present = is_present()
        smooth_ref[jnp.where(flip, blocks + 1, 0)] = jnp.where(present, got, jnp.zeros_like(got))
        start = jnp.where(flip, blocks - 1, 0)

    def body(i):
        c = start + i
        lhs = jnp.concatenate([smooth_ref[c], smooth_ref[c + 1], smooth_ref[c + 2]], axis=1)
        returned = jnp.dot(lhs, table_ref[c], preferred_element_type=F32)
        here = pl.ds(pl.multiple_of(c * CHUNK, CHUNK), CHUNK)
        anom = anom_ref[:, :, here].astype(F32)
        value = jnp.sum(anom * returned.reshape(anom.shape), axis=0)
        lane = pl.multiple_of(lax.rem(c, per) * CHUNK, CHUNK)
        place = lax.div(c, per) - lax.axis_index("mem")
        place = jnp.where(place < 0, place + shares, place)
        out_ref[place, :, pl.ds(lane, CHUNK)] = value.astype(BF16)

    groups(steps, unroll, body)


def back_call(part, steps, unroll, shares, got, table, anom, smooth, out=None):
    chunks, fields = table.shape[0], anom.shape[1]
    per = chunks // shares
    operands = ([] if part == 1 else [got]) + [table, anom, smooth]
    in_specs = [IN_VMEM] * len(operands)
    out_type = VMEM((shares, fields, per * CHUNK), BF16)
    if part == 2:
        out_type = jax.ShapeDtypeStruct(out_type.shape, BF16)
    smooth_type = VMEM(smooth.shape, BF16)
    last = len(operands) - 1
    if part == 0:
        out_shape, aliases = [smooth_type, out_type], {last: 0}
    elif part == 1:
        operands, in_specs = operands + [out], in_specs + [IN_VMEM]
        out_shape, aliases = [out_type], {last + 1: 0}
    else:
        operands, in_specs = operands + [out], in_specs + [IN_VMEM]
        out_shape, aliases = [smooth_type, out_type], {last: 0, last + 1: 1}
    return call(
        functools.partial(back_kernel, part, steps, unroll, per),
        in_specs,
        [IN_VMEM] * len(out_shape),
        out_shape,
        [],
        aliases,
    )(*operands)


def swaps(count, shares):
    inner, outer = [], []
    for i in range(count):
        far = i + 1 if i % 2 else i - 1
        for m in range(shares):
            here = i * shares + m
            inner.append((here, (i ^ 1) * shares + m))
            outer.append((here, far * shares + m if 0 <= far < count else i * shares + (m ^ 1)))
    return inner, outer


def swap(value, pairs):
    return lax.ppermute(value, ("space", "mem"), pairs)


def shards(increment, anomalies, interp_index, interp_weight, neighbour_blocks, tiles):
    members, _, columns = anomalies.shape
    chunks = columns // CHUNK
    count = lax.axis_size("space")
    shares = lax.axis_size("mem")
    assert count % 2 == 0 and shares % 2 == 0
    inner, outer = swaps(count, shares)
    head = chunks // 2 + 1
    table, own_near, carry, anom, *columns_here, neighbours = spread_first_call(
        NEAR, increment, anomalies, interp_index, interp_weight, neighbour_blocks
    )
    columns_here = (anom, *columns_here)
    got_near = swap(own_near, outer)
    table, own_far, carry = spread_more_call(NEAR, head - NEAR, table, carry, columns_here)
    got_far = swap(own_far, outer)
    table, own_a = spread_more_call(head, chunks - head, table, carry, columns_here)
    got_a = swap(own_a, inner)
    early = chunks - head - 1
    wide, smooth, edge_a = edge_early_call(
        neighbours, own_a, own_near, own_far, got_a, tiles
    )
    halo_a = swap(edge_a, inner)
    smooth = rest_call(True, early, early, neighbours, wide, tiles, smooth)
    smooth, out = back_call(0, early, early, shares, halo_a, table, anom, smooth)
    wide, smooth, edge_b = edge_late_call(neighbours, got_near, got_far, tiles, wide, smooth)
    halo_b = swap(edge_b, outer)
    smooth = rest_call(False, head - 1, head - 1, neighbours, wide, tiles, smooth)
    (out,) = back_call(1, head, head, shares, None, table, anom, smooth, out)
    _, pieces = back_call(2, 1, 1, shares, halo_b, table, anom, smooth, out)
    total = pieces[0].astype(F32)
    for shift in range(1, shares):
        pairs = [(i, (i + shift) % shares) for i in range(shares)]
        got = lax.ppermute(pieces[shift], "mem", pairs)
        total = total + got.astype(F32)
    return total / (members * shares - 1)


def solution(mesh):
    in_specs = (
        P(None, "space"),
        P("mem", None, "space"),
        P(None, "space"),
        P(None, "space"),
        P(None, "space"),
        P("space", None, None, None),
    )
    out_specs = P(None, ("space", "mem"))
    return jax.shard_map(shards, mesh=mesh, in_specs=in_specs, out_specs=out_specs, check_vma=False)
```

```python
import functools

import jax
import jax.numpy as jnp
from jax import lax
from jax.experimental import pallas as pl
from jax.experimental.pallas import tpu as pltpu
from jax.sharding import PartitionSpec as P


BLOCK = 128
HI = 128
RATIO = 4
CHUNK = RATIO * BLOCK
WIN = 3 * BLOCK
REACH = 2 * HI + 32
F32 = jnp.float32
BF16 = jnp.bfloat16
NEAR = 4
VMEM = pltpu.VMEM
ANY = pl.BlockSpec(memory_space=pl.ANY)
IN_VMEM = pl.BlockSpec(memory_space=pltpu.VMEM)
IN_SMEM = pl.BlockSpec(memory_space=pltpu.SMEM)


def is_present():
    space = lax.axis_index("space")
    last = lax.axis_size("space") - 1
    return jnp.where((space & 1) == 1, space < last, space > 0)


def in_hbm(x):
    return pltpu.with_memory_space_constraint(x, pltpu.HBM)


def call(kernel, in_specs, out_specs, out_shape, scratch, aliases=None):
    return pl.pallas_call(
        kernel,
        in_specs=in_specs,
        out_specs=out_specs,
        out_shape=out_shape,
        scratch_shapes=scratch,
        input_output_aliases=aliases or {},
        compiler_params=pltpu.CompilerParams(vmem_limit_bytes=16 * 1024 * 1024),
        cost_estimate=pl.CostEstimate(flops=0, bytes_accessed=0, transcendentals=0),
    )


def build_table(local, weight):
    i0, i1, i2 = local[0:1], local[1:2], local[2:3]
    w0, w1, w2 = weight[0:1], weight[1:2], weight[2:3]
    zero = jnp.zeros_like(w0)
    w0 = w0 + jnp.where(i1 == i0, w1, zero) + jnp.where(i2 == i0, w2, zero)
    w1 = w1 + jnp.where(i2 == i1, w2, zero)
    rows = REACH // 16
    iota = lax.broadcasted_iota(jnp.int32, (rows, 16, BLOCK), 0) * 16 + lax.broadcasted_iota(
        jnp.int32, (rows, 16, BLOCK), 1
    )
    iota = iota.astype(jnp.int16)
    parts = []
    for s in range(CHUNK // BLOCK):
        cols = slice(s * BLOCK, (s + 1) * BLOCK)
        base = s * BLOCK // RATIO

        def wide(x, kind):
            return jnp.broadcast_to(x[:, cols], (16, BLOCK)).astype(kind)[None]

        table = jnp.zeros((1, 16, BLOCK), BF16)
        for index, value in ((i2, w2), (i1, w1), (i0, w0)):
            table = jnp.where(wide(index - base, jnp.int16) == iota, wide(value, BF16), table)
        pieces = [table.reshape(REACH, BLOCK)]
        if base:
            pieces.insert(0, jnp.zeros((base, BLOCK), BF16))
        if base + REACH < WIN:
            pieces.append(jnp.zeros((WIN - base - REACH, BLOCK), BF16))
        parts.append(jnp.concatenate(pieces, axis=0))
    return jnp.concatenate(parts, axis=1)


def is_flipped():
    return (lax.axis_index("space") & 1) == 1


def spread_kernel(steps, done, chunks, *refs):
    first, last = done == 0, done + steps == chunks
    if first:
        anom_hbm, incr_hbm, index_hbm, weight_hbm, nbr_hbm = refs[:5]
        table_ref, out_ref, carry_ref = refs[5:8]
        anom_ref, incr_ref, index_ref, weight_ref, nbr_ref = refs[8:13]
        anom_sem, incr_sem, some_sem = refs[13:]
    else:
        anom_ref, incr_ref, index_ref, weight_ref, carry_in = refs[:5]
        table_ref, out_ref = refs[6:8]
        carry_ref = refs[-1]
    flip = is_flipped()

    def chunk_of(step):
        return jnp.where(flip, chunks - 1 - step, step)

    def lanes(c):
        return pl.ds(pl.multiple_of(c * CHUNK, CHUNK), CHUNK)

    if first:
        copies = [
            pltpu.make_async_copy(source, target, some_sem.at[k])
            for k, (source, target) in enumerate(
                ((index_hbm, index_ref), (weight_hbm, weight_ref), (nbr_hbm, nbr_ref))
            )
        ]
        columns = []
        for k, (begin, end) in enumerate(((0, steps), (steps, chunks))):
            low = jnp.where(flip, chunks - end, begin)
            here = pl.ds(pl.multiple_of(low * CHUNK, CHUNK), (end - begin) * CHUNK)
            columns.append(
                (
                    pltpu.make_async_copy(
                        anom_hbm.at[:, :, here], anom_ref.at[:, :, here], anom_sem.at[k]
                    ),
                    pltpu.make_async_copy(
                        incr_hbm.at[:, here], incr_ref.at[:, here], incr_sem.at[k]
                    ),
                )
            )
        for copy in (*copies[:2], *columns[0], *columns[1], copies[2]):
            copy.start()
        acc0 = acc1 = jnp.zeros(carry_ref.shape[1:], F32)
        for copy in copies[:2]:
            copy.wait()
    else:
        acc0, acc1 = carry_in[0], carry_in[1]
    rows = anom_ref.shape[0] * anom_ref.shape[1]
    total = out_ref.shape[0]

    def table_of(i):
        c = chunk_of(done + i)
        table = build_table(index_ref[:, lanes(c)] - c * BLOCK, weight_ref[:, lanes(c)])
        table_ref[c] = table
        return table

    before = steps if first else 0
    if first:
        for i in range(before):
            table_of(i)
        for copy in columns[0]:
            copy.wait()
    for i in range(steps):
        c = chunk_of(done + i)
        table = table_ref[c] if i < before else table_of(i)
        weighted = (anom_ref[:, :, lanes(c)].astype(F32) * incr_ref[:, lanes(c)][None]).astype(BF16)
        window = lax.dot_general(
            table,
            weighted.reshape(rows, CHUNK),
            (((1,), (1,)), ((), ())),
            preferred_element_type=F32,
        )
        near, mid, far = window[:BLOCK], window[BLOCK : 2 * BLOCK], window[2 * BLOCK :]
        ready = acc0 + jnp.where(flip, far, near)
        out_ref[jnp.where(flip, total - 1 - i, i)] = ready.T.astype(BF16)
        acc0 = acc1 + mid
        acc1 = jnp.where(flip, near, far)
    if last:
        out_ref[jnp.where(flip, 1, steps)] = acc0.T.astype(BF16)
        out_ref[jnp.where(flip, 0, steps + 1)] = acc1.T.astype(BF16)
    else:
        carry_ref[0] = acc0
        carry_ref[1] = acc1
    if first:
        for copy in (*columns[1], copies[2]):
            copy.wait()


def spread_first_call(steps, increment, anomalies, index, weight, neighbours):
    members, fields, columns = anomalies.shape
    rows = members * fields
    chunks = columns // CHUNK
    return call(
        functools.partial(spread_kernel, steps, 0, chunks),
        [ANY] * 5,
        [IN_VMEM] * 7 + [IN_SMEM],
        [
            VMEM((chunks, WIN, CHUNK), BF16),
            jax.ShapeDtypeStruct((steps, rows, BLOCK), BF16),
            VMEM((2, BLOCK, rows), F32),
            VMEM(anomalies.shape, BF16),
            VMEM(increment.shape, F32),
            VMEM(index.shape, jnp.int32),
            VMEM(weight.shape, F32),
            pltpu.SMEM(neighbours.shape, jnp.int32),
        ],
        [
            pltpu.SemaphoreType.DMA((2,)),
            pltpu.SemaphoreType.DMA((2,)),
            pltpu.SemaphoreType.DMA((3,)),
        ],
    )(*(in_hbm(x) for x in (anomalies, increment, index, weight, neighbours)))


def spread_more_call(done, steps, table, carry, columns):
    chunks = table.shape[0]
    rows = carry.shape[2]
    last = done + steps == chunks
    out_shape = [
        VMEM(table.shape, BF16),
        jax.ShapeDtypeStruct((steps + 2 * last, rows, BLOCK), BF16),
    ]
    if not last:
        out_shape.append(VMEM(carry.shape, F32))
    return call(
        functools.partial(spread_kernel, steps, done, chunks),
        [IN_VMEM] * 6,
        [IN_VMEM] * len(out_shape),
        out_shape,
        [],
        {5: 0},
    )(*columns, carry, table)


def convolve(wide_ref, tiles_ref, nbr_ref, b):
    count = tiles_ref.shape[1]
    picked = jnp.concatenate([wide_ref[nbr_ref[n, b]] for n in range(count)], axis=1)
    weights = tiles_ref[b].reshape(count * BLOCK, BLOCK)
    return jnp.dot(picked, weights, preferred_element_type=F32).astype(BF16)


def edge_early_kernel(
    nbr_ref, own_a, own_near, own_far, got_a, tiles_ref, wide_ref, smooth_ref, edge_ref
):
    half = own_a.shape[0]
    near = own_near.shape[0]
    reach = half - 1
    blocks = tiles_ref.shape[0]
    top = blocks + reach
    flip = is_flipped()

    @pl.when(jnp.logical_not(flip))
    def _():
        wide_ref[reach - 1 : reach - 1 + near] = own_near[...]
        wide_ref[reach - 1 + near : reach - 1 + half] = own_far[...]
        wide_ref[reach - 1 + half : top - 1] = own_a[0 : half - 2]
        wide_ref[top - 1 : top + 1] = (
            got_a[0:2].astype(F32) + own_a[half - 2 : half].astype(F32)
        ).astype(BF16)
        wide_ref[top + 1 : top + reach] = got_a[2:half]

    @pl.when(flip)
    def _():
        wide_ref[0 : reach - 1] = got_a[0 : reach - 1]
        wide_ref[reach - 1 : reach + 1] = (
            got_a[reach - 1 : reach + 1].astype(F32) + own_a[0:2].astype(F32)
        ).astype(BF16)
        wide_ref[reach + 1 : reach - 1 + half] = own_a[2:half]
        wide_ref[reach - 1 + half : top + 1 - near] = own_far[...]
        wide_ref[top + 1 - near : top + 1] = own_near[...]

    b = jnp.where(flip, 0, blocks - 1)
    edge = convolve(wide_ref, tiles_ref, nbr_ref, b)
    smooth_ref[b + 1] = edge
    edge_ref[...] = edge


def edge_late_kernel(
    nbr_ref, got_near, got_far, tiles_ref, wide_in, smooth_in, wide_ref, smooth_ref, edge_ref
):
    near = got_near.shape[0]
    half = near + got_far.shape[0]
    reach = half - 1
    blocks = tiles_ref.shape[0]
    top = blocks + reach
    flip = is_flipped()
    present = is_present()

    def there(value):
        return jnp.where(present, value, jnp.zeros_like(value))

    @pl.when(jnp.logical_not(flip))
    def _():
        wide_ref[0 : half - near] = there(got_far[...])
        wide_ref[half - near : reach - 1] = there(got_near[0 : near - 2])
        both = wide_ref[reach - 1 : reach + 1].astype(F32) + there(got_near[near - 2 :].astype(F32))
        wide_ref[reach - 1] = there(both[0]).astype(BF16)
        wide_ref[reach] = both[1].astype(BF16)

    @pl.when(flip)
    def _():
        both = wide_ref[top - 1 : top + 1].astype(F32) + there(got_near[0:2].astype(F32))
        wide_ref[top - 1] = both[0].astype(BF16)
        wide_ref[top] = there(both[1]).astype(BF16)
        wide_ref[top + 1 : top - 1 + near] = there(got_near[2:near])
        wide_ref[top - 1 + near : top + reach] = there(got_far[...])

    b = jnp.where(flip, blocks - 1, 0)
    edge = convolve(wide_ref, tiles_ref, nbr_ref, b)
    smooth_ref[b + 1] = edge
    edge_ref[...] = edge


def back_chunk(smooth_ref, table_ref, anom_ref, out_ref, c):
    shares = out_ref.shape[0]
    per = table_ref.shape[0] // shares
    lhs = jnp.concatenate([smooth_ref[c], smooth_ref[c + 1], smooth_ref[c + 2]], axis=1)
    returned = jnp.dot(lhs, table_ref[c], preferred_element_type=F32)
    here = pl.ds(pl.multiple_of(c * CHUNK, CHUNK), CHUNK)
    anom = anom_ref[:, :, here].astype(F32)
    value = jnp.sum(anom * returned.reshape(anom.shape), axis=0)
    place = lax.div(c, per) - lax.axis_index("mem")
    place = jnp.where(place < 0, place + shares, place)
    lane = pl.multiple_of(lax.rem(c, per) * CHUNK, CHUNK)
    out_ref[place, :, pl.ds(lane, CHUNK)] = value.astype(BF16)


def early_kernel(
    steps, nbr_ref, wide_ref, tiles_ref, table_ref, anom_ref, smooth_in, smooth_ref, out_ref
):
    blocks = tiles_ref.shape[0]
    flip = is_flipped()
    start = jnp.where(flip, 1, blocks - 1 - steps)
    for i in range(steps):
        smooth_ref[start + i + 1] = convolve(wide_ref, tiles_ref, nbr_ref, start + i)
    start = jnp.where(flip, 1, blocks - steps)
    for i in range(steps - 1):
        back_chunk(smooth_ref, table_ref, anom_ref, out_ref, start + i)


def late_kernel(
    steps,
    nbr_ref,
    halo_ref,
    wide_ref,
    tiles_ref,
    table_ref,
    anom_ref,
    smooth_in,
    out_in,
    smooth_ref,
    out_ref,
    main_ref,
):
    blocks = tiles_ref.shape[0]
    flip = is_flipped()
    start = jnp.where(flip, blocks - 1 - steps, 1)
    for i in range(steps):
        smooth_ref[start + i + 1] = convolve(wide_ref, tiles_ref, nbr_ref, start + i)
    smooth_ref[jnp.where(flip, 0, blocks + 1)] = halo_ref[...]
    back_chunk(smooth_ref, table_ref, anom_ref, out_ref, jnp.where(flip, 0, blocks - 1))
    start = jnp.where(flip, blocks - 2 - steps, 1)
    for i in range(steps + 1):
        back_chunk(smooth_ref, table_ref, anom_ref, out_ref, start + i)
    width = main_ref.shape[1]
    here = pl.ds(pl.multiple_of(jnp.where(flip, 0, CHUNK), CHUNK), width)
    main_ref[...] = out_ref[out_ref.shape[0] // 2, :, here]


def last_kernel(
    halo_ref, table_ref, anom_ref, smooth_in, out_in, smooth_ref, out_ref, edge_ref
):
    blocks = table_ref.shape[0]
    flip = is_flipped()
    halo = halo_ref[...]
    smooth_ref[jnp.where(flip, blocks + 1, 0)] = jnp.where(is_present(), halo, jnp.zeros_like(halo))
    back_chunk(smooth_ref, table_ref, anom_ref, out_ref, jnp.where(flip, blocks - 1, 0))
    shares, _, columns = out_ref.shape
    here = pl.ds(pl.multiple_of(jnp.where(flip, columns - CHUNK, 0), CHUNK), CHUNK)
    edge_ref[...] = out_ref[shares // 2, :, here]


def edge_early_call(neighbours, own_a, own_near, own_far, got_a, tiles):
    blocks = tiles.shape[0]
    half, rows, _ = own_a.shape
    return call(
        edge_early_kernel,
        [IN_SMEM] + [IN_VMEM] * 5,
        [IN_VMEM] * 3,
        [
            VMEM((blocks + 2 * half - 2, rows, BLOCK), BF16),
            VMEM((blocks + 2, rows, BLOCK), BF16),
            jax.ShapeDtypeStruct((rows, BLOCK), BF16),
        ],
        [],
    )(neighbours, own_a, own_near, own_far, got_a, tiles)


def edge_late_call(neighbours, got_near, got_far, tiles, wide, smooth):
    _, rows, _ = got_near.shape
    return call(
        edge_late_kernel,
        [IN_SMEM] + [IN_VMEM] * 5,
        [IN_VMEM] * 3,
        [
            VMEM(wide.shape, BF16),
            VMEM(smooth.shape, BF16),
            jax.ShapeDtypeStruct((rows, BLOCK), BF16),
        ],
        [],
        {4: 0, 5: 1},
    )(neighbours, got_near, got_far, tiles, wide, smooth)


def early_call(steps, shares, neighbours, wide, tiles, table, anom, smooth):
    _, fields, columns = anom.shape
    return call(
        functools.partial(early_kernel, steps),
        [IN_SMEM] + [IN_VMEM] * 5,
        [IN_VMEM] * 2,
        [VMEM(smooth.shape, BF16), VMEM((shares, fields, columns // shares), BF16)],
        [],
        {5: 0},
    )(neighbours, wide, tiles, table, anom, smooth)


def late_call(steps, neighbours, halo, wide, tiles, table, anom, smooth, out):
    return call(
        functools.partial(late_kernel, steps),
        [IN_SMEM] + [IN_VMEM] * 7,
        [IN_VMEM] * 3,
        [
            VMEM(smooth.shape, BF16),
            VMEM(out.shape, BF16),
            jax.ShapeDtypeStruct((out.shape[1], out.shape[2] - CHUNK), BF16),
        ],
        [],
        {6: 0, 7: 1},
    )(neighbours, halo, wide, tiles, table, anom, smooth, out)


def last_call(halo, table, anom, smooth, out):
    return call(
        last_kernel,
        [IN_VMEM] * 5,
        [IN_VMEM] * 3,
        [
            VMEM(smooth.shape, BF16),
            jax.ShapeDtypeStruct(out.shape, BF16),
            jax.ShapeDtypeStruct((out.shape[1], CHUNK), BF16),
        ],
        [],
        {3: 0, 4: 1},
    )(halo, table, anom, smooth, out)


def swaps(count, shares):
    inner, outer = [], []
    for i in range(count):
        far = i + 1 if i % 2 else i - 1
        for m in range(shares):
            here = i * shares + m
            inner.append((here, (i ^ 1) * shares + m))
            outer.append((here, far * shares + m if 0 <= far < count else i * shares + (m ^ 1)))
    return inner, outer


def swap(value, pairs):
    return lax.ppermute(value, ("space", "mem"), pairs)


def pass_on(value, shift, shares):
    return lax.ppermute(value, "mem", [(i, (i + shift) % shares) for i in range(shares)])


def shards(increment, anomalies, interp_index, interp_weight, neighbour_blocks, tiles):
    members, _, columns = anomalies.shape
    chunks = columns // CHUNK
    count = lax.axis_size("space")
    shares = lax.axis_size("mem")
    assert count % 2 == 0 and shares % 2 == 0 and chunks > shares
    inner, outer = swaps(count, shares)
    head = chunks // 2 + 1
    table, own_near, carry, anom, *columns_here, neighbours = spread_first_call(
        NEAR, increment, anomalies, interp_index, interp_weight, neighbour_blocks
    )
    columns_here = (anom, *columns_here)
    got_near = swap(own_near, outer)
    table, own_far, carry = spread_more_call(NEAR, head - NEAR, table, carry, columns_here)
    got_far = swap(own_far, outer)
    table, own_a = spread_more_call(head, chunks - head, table, carry, columns_here)
    got_a = swap(own_a, inner)
    early = chunks - head - 1
    wide, smooth, edge_a = edge_early_call(
        neighbours, own_a, own_near, own_far, got_a, tiles
    )
    halo_a = swap(edge_a, inner)
    smooth, out = early_call(early, shares, neighbours, wide, tiles, table, anom, smooth)
    wide, smooth, edge_b = edge_late_call(neighbours, got_near, got_far, tiles, wide, smooth)
    halo_b = swap(edge_b, outer)
    smooth, out, main = late_call(
        head - 1, neighbours, halo_a, wide, tiles, table, anom, smooth, out
    )
    half = shares // 2
    main = pass_on(main, half, shares)
    _, pieces, edge = last_call(halo_b, table, anom, smooth, out)
    total = pieces[0].astype(F32)
    for shift in range(1, shares):
        piece = edge if shift == half else pieces[shift]
        got = pass_on(piece, shift, shares)
        if shift == half:
            flip = is_flipped()
            got = jnp.where(
                flip,
                jnp.concatenate([main, got], axis=1),
                jnp.concatenate([got, main], axis=1),
            )
        total = total + got.astype(F32)
    return total / (members * shares - 1)


def solution(mesh):
    in_specs = (
        P(None, "space"),
        P("mem", None, "space"),
        P(None, "space"),
        P(None, "space"),
        P(None, "space"),
        P("space", None, None, None),
    )
    out_specs = P(None, ("space", "mem"))
    return jax.shard_map(shards, mesh=mesh, in_specs=in_specs, out_specs=out_specs, check_vma=False)
```

```python
import functools

import jax
import jax.numpy as jnp
from jax import lax
from jax.experimental import pallas as pl
from jax.experimental.pallas import tpu as pltpu
from jax.sharding import PartitionSpec as P


BLOCK = 128
HI = 128
RATIO = 4
CHUNK = RATIO * BLOCK
WIN = 3 * BLOCK
REACH = 2 * HI + 32
F32 = jnp.float32
BF16 = jnp.bfloat16
NEAR = 5
VMEM = pltpu.VMEM
ANY = pl.BlockSpec(memory_space=pl.ANY)
IN_VMEM = pl.BlockSpec(memory_space=pltpu.VMEM)
IN_SMEM = pl.BlockSpec(memory_space=pltpu.SMEM)


def is_present():
    space = lax.axis_index("space")
    last = lax.axis_size("space") - 1
    return jnp.where((space & 1) == 1, space < last, space > 0)


def in_hbm(x):
    return pltpu.with_memory_space_constraint(x, pltpu.HBM)


def call(kernel, in_specs, out_specs, out_shape, scratch, aliases=None):
    return pl.pallas_call(
        kernel,
        in_specs=in_specs,
        out_specs=out_specs,
        out_shape=out_shape,
        scratch_shapes=scratch,
        input_output_aliases=aliases or {},
        compiler_params=pltpu.CompilerParams(vmem_limit_bytes=16 * 1024 * 1024),
        cost_estimate=pl.CostEstimate(flops=0, bytes_accessed=0, transcendentals=0),
    )


def build_table(local, weight):
    i0, i1, i2 = local[0:1], local[1:2], local[2:3]
    w0, w1, w2 = weight[0:1], weight[1:2], weight[2:3]
    zero = jnp.zeros_like(w0)
    w0 = w0 + jnp.where(i1 == i0, w1, zero) + jnp.where(i2 == i0, w2, zero)
    w1 = w1 + jnp.where(i2 == i1, w2, zero)
    rows = REACH // 16
    iota = lax.broadcasted_iota(jnp.int32, (rows, 16, BLOCK), 0) * 16 + lax.broadcasted_iota(
        jnp.int32, (rows, 16, BLOCK), 1
    )
    iota = iota.astype(jnp.int16)
    parts = []
    for s in range(CHUNK // BLOCK):
        cols = slice(s * BLOCK, (s + 1) * BLOCK)
        base = s * BLOCK // RATIO

        def wide(x, kind):
            return jnp.broadcast_to(x[:, cols], (16, BLOCK)).astype(kind)[None]

        table = jnp.zeros((1, 16, BLOCK), BF16)
        for index, value in ((i2, w2), (i1, w1), (i0, w0)):
            table = jnp.where(wide(index - base, jnp.int16) == iota, wide(value, BF16), table)
        pieces = [table.reshape(REACH, BLOCK)]
        if base:
            pieces.insert(0, jnp.zeros((base, BLOCK), BF16))
        if base + REACH < WIN:
            pieces.append(jnp.zeros((WIN - base - REACH, BLOCK), BF16))
        parts.append(jnp.concatenate(pieces, axis=0))
    return jnp.concatenate(parts, axis=1)


def is_flipped():
    return (lax.axis_index("space") & 1) == 1


def spread_kernel(steps, done, chunks, *refs):
    first, last = done == 0, done + steps == chunks
    if first:
        anom_hbm, incr_hbm, index_hbm, weight_hbm, nbr_hbm = refs[:5]
        table_ref, out_ref, carry_ref = refs[5:8]
        anom_ref, incr_ref, index_ref, weight_ref, nbr_ref = refs[8:13]
        anom_sem, incr_sem, some_sem = refs[13:]
    else:
        anom_ref, incr_ref, index_ref, weight_ref, carry_in = refs[:5]
        table_ref, out_ref = refs[6:8]
        carry_ref = refs[-1]
    flip = is_flipped()

    def chunk_of(step):
        return jnp.where(flip, chunks - 1 - step, step)

    def lanes(c):
        return pl.ds(pl.multiple_of(c * CHUNK, CHUNK), CHUNK)

    if first:
        copies = [
            pltpu.make_async_copy(source, target, some_sem.at[k])
            for k, (source, target) in enumerate(
                ((index_hbm, index_ref), (weight_hbm, weight_ref), (nbr_hbm, nbr_ref))
            )
        ]
        columns = []
        for k, (begin, end) in enumerate(((0, steps), (steps, chunks))):
            low = jnp.where(flip, chunks - end, begin)
            here = pl.ds(pl.multiple_of(low * CHUNK, CHUNK), (end - begin) * CHUNK)
            columns.append(
                (
                    pltpu.make_async_copy(
                        anom_hbm.at[:, :, here], anom_ref.at[:, :, here], anom_sem.at[k]
                    ),
                    pltpu.make_async_copy(
                        incr_hbm.at[:, here], incr_ref.at[:, here], incr_sem.at[k]
                    ),
                )
            )
        for copy in (*copies[:2], *columns[0], *columns[1], copies[2]):
            copy.start()
        acc0 = acc1 = jnp.zeros(carry_ref.shape[1:], F32)
        for copy in copies[:2]:
            copy.wait()
    else:
        acc0, acc1 = carry_in[0], carry_in[1]
    rows = anom_ref.shape[0] * anom_ref.shape[1]
    total = out_ref.shape[0]

    def table_of(i):
        c = chunk_of(done + i)
        table = build_table(index_ref[:, lanes(c)] - c * BLOCK, weight_ref[:, lanes(c)])
        table_ref[c] = table
        return table

    before = steps if first else 0
    if first:
        for i in range(before):
            table_of(i)
        for copy in columns[0]:
            copy.wait()
    for i in range(steps):
        c = chunk_of(done + i)
        table = table_ref[c] if i < before else table_of(i)
        weighted = (anom_ref[:, :, lanes(c)].astype(F32) * incr_ref[:, lanes(c)][None]).astype(BF16)
        window = lax.dot_general(
            table,
            weighted.reshape(rows, CHUNK),
            (((1,), (1,)), ((), ())),
            preferred_element_type=F32,
        )
        near, mid, far = window[:BLOCK], window[BLOCK : 2 * BLOCK], window[2 * BLOCK :]
        ready = acc0 + jnp.where(flip, far, near)
        out_ref[jnp.where(flip, total - 1 - i, i)] = ready.T.astype(BF16)
        acc0 = acc1 + mid
        acc1 = jnp.where(flip, near, far)
    if last:
        out_ref[jnp.where(flip, 1, steps)] = acc0.T.astype(BF16)
        out_ref[jnp.where(flip, 0, steps + 1)] = acc1.T.astype(BF16)
    else:
        carry_ref[0] = acc0
        carry_ref[1] = acc1
    if first:
        for copy in (*columns[1], copies[2]):
            copy.wait()


def spread_first_call(steps, increment, anomalies, index, weight, neighbours):
    members, fields, columns = anomalies.shape
    rows = members * fields
    chunks = columns // CHUNK
    return call(
        functools.partial(spread_kernel, steps, 0, chunks),
        [ANY] * 5,
        [IN_VMEM] * 7 + [IN_SMEM],
        [
            VMEM((chunks, WIN, CHUNK), BF16),
            jax.ShapeDtypeStruct((steps, rows, BLOCK), BF16),
            VMEM((2, BLOCK, rows), F32),
            VMEM(anomalies.shape, BF16),
            VMEM(increment.shape, F32),
            VMEM(index.shape, jnp.int32),
            VMEM(weight.shape, F32),
            pltpu.SMEM(neighbours.shape, jnp.int32),
        ],
        [
            pltpu.SemaphoreType.DMA((2,)),
            pltpu.SemaphoreType.DMA((2,)),
            pltpu.SemaphoreType.DMA((3,)),
        ],
    )(*(in_hbm(x) for x in (anomalies, increment, index, weight, neighbours)))


def spread_more_call(done, steps, table, carry, columns):
    chunks = table.shape[0]
    rows = carry.shape[2]
    last = done + steps == chunks
    out_shape = [
        VMEM(table.shape, BF16),
        jax.ShapeDtypeStruct((steps + 2 * last, rows, BLOCK), BF16),
    ]
    if not last:
        out_shape.append(VMEM(carry.shape, F32))
    return call(
        functools.partial(spread_kernel, steps, done, chunks),
        [IN_VMEM] * 6,
        [IN_VMEM] * len(out_shape),
        out_shape,
        [],
        {5: 0},
    )(*columns, carry, table)


def convolve(wide_ref, tiles_ref, nbr_ref, b):
    count = tiles_ref.shape[1]
    picked = jnp.concatenate([wide_ref[nbr_ref[n, b]] for n in range(count)], axis=1)
    weights = tiles_ref[b].reshape(count * BLOCK, BLOCK)
    return jnp.dot(picked, weights, preferred_element_type=F32).astype(BF16)


def edge_early_kernel(
    nbr_ref, own_a, own_near, own_far, got_a, tiles_ref, wide_ref, smooth_ref, edge_ref
):
    half = own_a.shape[0]
    near = own_near.shape[0]
    reach = half - 1
    blocks = tiles_ref.shape[0]
    top = blocks + reach
    flip = is_flipped()

    @pl.when(jnp.logical_not(flip))
    def _():
        wide_ref[reach - 1 : reach - 1 + near] = own_near[...]
        wide_ref[reach - 1 + near : reach - 1 + half] = own_far[...]
        wide_ref[reach - 1 + half : top - 1] = own_a[0 : half - 2]
        wide_ref[top - 1 : top + 1] = (
            got_a[0:2].astype(F32) + own_a[half - 2 : half].astype(F32)
        ).astype(BF16)
        wide_ref[top + 1 : top + reach] = got_a[2:half]

    @pl.when(flip)
    def _():
        wide_ref[0 : reach - 1] = got_a[0 : reach - 1]
        wide_ref[reach - 1 : reach + 1] = (
            got_a[reach - 1 : reach + 1].astype(F32) + own_a[0:2].astype(F32)
        ).astype(BF16)
        wide_ref[reach + 1 : reach - 1 + half] = own_a[2:half]
        wide_ref[reach - 1 + half : top + 1 - near] = own_far[...]
        wide_ref[top + 1 - near : top + 1] = own_near[...]

    b = jnp.where(flip, 0, blocks - 1)
    edge = convolve(wide_ref, tiles_ref, nbr_ref, b)
    smooth_ref[b + 1] = edge
    edge_ref[...] = edge


def edge_late_kernel(
    nbr_ref, got_far, tiles_ref, wide_in, smooth_in, wide_ref, smooth_ref, edge_ref
):
    far = got_far.shape[0]
    blocks = tiles_ref.shape[0]
    flip = is_flipped()
    wide_ref[pl.ds(jnp.where(flip, wide_ref.shape[0] - far, 0), far)] = there(got_far[...])
    b = jnp.where(flip, blocks - 1, 0)
    edge = convolve(wide_ref, tiles_ref, nbr_ref, b)
    smooth_ref[b + 1] = edge
    edge_ref[...] = edge


def back_chunk(smooth_ref, table_ref, anom_ref, out_ref, c):
    shares = out_ref.shape[0]
    per = table_ref.shape[0] // shares
    lhs = jnp.concatenate([smooth_ref[c], smooth_ref[c + 1], smooth_ref[c + 2]], axis=1)
    returned = jnp.dot(lhs, table_ref[c], preferred_element_type=F32)
    here = pl.ds(pl.multiple_of(c * CHUNK, CHUNK), CHUNK)
    anom = anom_ref[:, :, here].astype(F32)
    value = jnp.sum(anom * returned.reshape(anom.shape), axis=0)
    place = lax.div(c, per) - lax.axis_index("mem")
    place = jnp.where(place < 0, place + shares, place)
    lane = pl.multiple_of(lax.rem(c, per) * CHUNK, CHUNK)
    out_ref[place, :, pl.ds(lane, CHUNK)] = value.astype(BF16)


def there(value):
    return jnp.where(is_present(), value, jnp.zeros_like(value))


def early_kernel(
    steps,
    nbr_ref,
    got_near,
    wide_in,
    tiles_ref,
    table_ref,
    anom_ref,
    smooth_in,
    wide_ref,
    smooth_ref,
    out_ref,
):
    blocks = tiles_ref.shape[0]
    near = got_near.shape[0]
    half = blocks - steps - 1
    reach = half - 1
    top = blocks + reach
    flip = is_flipped()
    start = jnp.where(flip, 1, blocks - 1 - steps)
    for i in range(steps):
        smooth_ref[start + i + 1] = convolve(wide_ref, tiles_ref, nbr_ref, start + i)

    @pl.when(jnp.logical_not(flip))
    def _():
        wide_ref[half - near : reach - 1] = there(got_near[0 : near - 2])
        both = wide_ref[reach - 1 : reach + 1].astype(F32) + there(got_near[near - 2 :].astype(F32))
        wide_ref[reach - 1] = there(both[0]).astype(BF16)
        wide_ref[reach] = both[1].astype(BF16)

    @pl.when(flip)
    def _():
        both = wide_ref[top - 1 : top + 1].astype(F32) + there(got_near[0:2].astype(F32))
        wide_ref[top - 1] = both[0].astype(BF16)
        wide_ref[top] = there(both[1]).astype(BF16)
        wide_ref[top + 1 : top - 1 + near] = there(got_near[2:near])

    start = jnp.where(flip, blocks - half, half - near)
    for i in range(near):
        smooth_ref[start + i + 1] = convolve(wide_ref, tiles_ref, nbr_ref, start + i)
    start = jnp.where(flip, 1, half - near + 1)
    for i in range(steps - 1 + near):
        back_chunk(smooth_ref, table_ref, anom_ref, out_ref, start + i)


def late_kernel(
    steps,
    nbr_ref,
    halo_ref,
    wide_ref,
    tiles_ref,
    table_ref,
    anom_ref,
    smooth_in,
    out_in,
    smooth_ref,
    out_ref,
    main_ref,
):
    blocks = tiles_ref.shape[0]
    flip = is_flipped()
    start = jnp.where(flip, blocks - 1 - steps, 1)
    for i in range(steps):
        smooth_ref[start + i + 1] = convolve(wide_ref, tiles_ref, nbr_ref, start + i)
    start = jnp.where(flip, blocks - 2 - steps, 1)
    smooth_ref[jnp.where(flip, 0, blocks + 1)] = halo_ref[...]
    back_chunk(smooth_ref, table_ref, anom_ref, out_ref, jnp.where(flip, 0, blocks - 1))
    for i in range(steps + 1):
        back_chunk(smooth_ref, table_ref, anom_ref, out_ref, start + i)
    width = main_ref.shape[1]
    here = pl.ds(pl.multiple_of(jnp.where(flip, 0, CHUNK), CHUNK), width)
    main_ref[...] = out_ref[out_ref.shape[0] // 2, :, here]


def last_kernel(
    halo_ref, table_ref, anom_ref, smooth_in, out_in, smooth_ref, out_ref, edge_ref
):
    blocks = table_ref.shape[0]
    flip = is_flipped()
    halo = halo_ref[...]
    smooth_ref[jnp.where(flip, blocks + 1, 0)] = jnp.where(is_present(), halo, jnp.zeros_like(halo))
    back_chunk(smooth_ref, table_ref, anom_ref, out_ref, jnp.where(flip, blocks - 1, 0))
    shares, _, columns = out_ref.shape
    here = pl.ds(pl.multiple_of(jnp.where(flip, columns - CHUNK, 0), CHUNK), CHUNK)
    edge_ref[...] = out_ref[shares // 2, :, here]


def edge_early_call(neighbours, own_a, own_near, own_far, got_a, tiles):
    blocks = tiles.shape[0]
    half, rows, _ = own_a.shape
    return call(
        edge_early_kernel,
        [IN_SMEM] + [IN_VMEM] * 5,
        [IN_VMEM] * 3,
        [
            VMEM((blocks + 2 * half - 2, rows, BLOCK), BF16),
            VMEM((blocks + 2, rows, BLOCK), BF16),
            jax.ShapeDtypeStruct((rows, BLOCK), BF16),
        ],
        [],
    )(neighbours, own_a, own_near, own_far, got_a, tiles)


def edge_late_call(neighbours, got_far, tiles, wide, smooth):
    _, rows, _ = got_far.shape
    return call(
        edge_late_kernel,
        [IN_SMEM] + [IN_VMEM] * 4,
        [IN_VMEM] * 3,
        [
            VMEM(wide.shape, BF16),
            VMEM(smooth.shape, BF16),
            jax.ShapeDtypeStruct((rows, BLOCK), BF16),
        ],
        [],
        {3: 0, 4: 1},
    )(neighbours, got_far, tiles, wide, smooth)


def early_call(steps, shares, neighbours, got_near, wide, tiles, table, anom, smooth):
    _, fields, columns = anom.shape
    return call(
        functools.partial(early_kernel, steps),
        [IN_SMEM] + [IN_VMEM] * 6,
        [IN_VMEM] * 3,
        [
            VMEM(wide.shape, BF16),
            VMEM(smooth.shape, BF16),
            VMEM((shares, fields, columns // shares), BF16),
        ],
        [],
        {2: 0, 6: 1},
    )(neighbours, got_near, wide, tiles, table, anom, smooth)


def late_call(steps, neighbours, halo, wide, tiles, table, anom, smooth, out):
    return call(
        functools.partial(late_kernel, steps),
        [IN_SMEM] + [IN_VMEM] * 7,
        [IN_VMEM] * 3,
        [
            VMEM(smooth.shape, BF16),
            VMEM(out.shape, BF16),
            jax.ShapeDtypeStruct((out.shape[1], out.shape[2] - CHUNK), BF16),
        ],
        [],
        {6: 0, 7: 1},
    )(neighbours, halo, wide, tiles, table, anom, smooth, out)


def last_call(halo, table, anom, smooth, out):
    return call(
        last_kernel,
        [IN_VMEM] * 5,
        [IN_VMEM] * 3,
        [
            VMEM(smooth.shape, BF16),
            jax.ShapeDtypeStruct(out.shape, BF16),
            jax.ShapeDtypeStruct((out.shape[1], CHUNK), BF16),
        ],
        [],
        {3: 0, 4: 1},
    )(halo, table, anom, smooth, out)


def swaps(count, shares):
    inner, outer = [], []
    for i in range(count):
        far = i + 1 if i % 2 else i - 1
        for m in range(shares):
            here = i * shares + m
            inner.append((here, (i ^ 1) * shares + m))
            outer.append((here, far * shares + m if 0 <= far < count else i * shares + (m ^ 1)))
    return inner, outer


def swap(value, pairs):
    return lax.ppermute(value, ("space", "mem"), pairs)


def pass_on(value, shift, shares):
    return lax.ppermute(value, "mem", [(i, (i + shift) % shares) for i in range(shares)])


def shards(increment, anomalies, interp_index, interp_weight, neighbour_blocks, tiles):
    members, _, columns = anomalies.shape
    chunks = columns // CHUNK
    count = lax.axis_size("space")
    shares = lax.axis_size("mem")
    assert count % 2 == 0 and shares % 2 == 0 and chunks > shares
    inner, outer = swaps(count, shares)
    head = chunks // 2 + 1
    table, own_near, carry, anom, *columns_here, neighbours = spread_first_call(
        NEAR, increment, anomalies, interp_index, interp_weight, neighbour_blocks
    )
    columns_here = (anom, *columns_here)
    got_near = swap(own_near, outer)
    table, own_far, carry = spread_more_call(NEAR, head - NEAR, table, carry, columns_here)
    got_far = swap(own_far, outer)
    table, own_a = spread_more_call(head, chunks - head, table, carry, columns_here)
    got_a = swap(own_a, inner)
    early = chunks - head - 1
    wide, smooth, edge_a = edge_early_call(
        neighbours, own_a, own_near, own_far, got_a, tiles
    )
    halo_a = swap(edge_a, inner)
    wide, smooth, out = early_call(
        early, shares, neighbours, got_near, wide, tiles, table, anom, smooth
    )
    wide, smooth, edge_b = edge_late_call(neighbours, got_far, tiles, wide, smooth)
    halo_b = swap(edge_b, outer)
    smooth, out, main = late_call(
        head - 1 - NEAR, neighbours, halo_a, wide, tiles, table, anom, smooth, out
    )
    half = shares // 2
    main = pass_on(main, half, shares)
    _, pieces, edge = last_call(halo_b, table, anom, smooth, out)
    total = pieces[0].astype(F32)
    for shift in range(1, shares):
        piece = edge if shift == half else pieces[shift]
        got = pass_on(piece, shift, shares)
        if shift == half:
            flip = is_flipped()
            got = jnp.where(
                flip,
                jnp.concatenate([main, got], axis=1),
                jnp.concatenate([got, main], axis=1),
            )
        total = total + got.astype(F32)
    return total / (members * shares - 1)


def solution(mesh):
    in_specs = (
        P(None, "space"),
        P("mem", None, "space"),
        P(None, "space"),
        P(None, "space"),
        P(None, "space"),
        P("space", None, None, None),
    )
    out_specs = P(None, ("space", "mem"))
    return jax.shard_map(shards, mesh=mesh, in_specs=in_specs, out_specs=out_specs, check_vma=False)
```

```python
import functools

import jax
import jax.numpy as jnp
from jax import lax
from jax.experimental import pallas as pl
from jax.experimental.pallas import tpu as pltpu
from jax.sharding import PartitionSpec as P


BLOCK = 128
HI = 128
RATIO = 4
CHUNK = RATIO * BLOCK
WIN = 3 * BLOCK
REACH = 2 * HI + 32
F32 = jnp.float32
BF16 = jnp.bfloat16
NEAR = 4
VMEM = pltpu.VMEM
ANY = pl.BlockSpec(memory_space=pl.ANY)
IN_VMEM = pl.BlockSpec(memory_space=pltpu.VMEM)
IN_SMEM = pl.BlockSpec(memory_space=pltpu.SMEM)


def is_present():
    space = lax.axis_index("space")
    last = lax.axis_size("space") - 1
    return jnp.where((space & 1) == 1, space < last, space > 0)


def in_hbm(x):
    return pltpu.with_memory_space_constraint(x, pltpu.HBM)


def call(kernel, in_specs, out_specs, out_shape, scratch, aliases=None):
    return pl.pallas_call(
        kernel,
        in_specs=in_specs,
        out_specs=out_specs,
        out_shape=out_shape,
        scratch_shapes=scratch,
        input_output_aliases=aliases or {},
        compiler_params=pltpu.CompilerParams(vmem_limit_bytes=16 * 1024 * 1024),
        cost_estimate=pl.CostEstimate(flops=0, bytes_accessed=0, transcendentals=0),
    )


def build_table(local, weight):
    i0, i1, i2 = local[0:1], local[1:2], local[2:3]
    w0, w1, w2 = weight[0:1], weight[1:2], weight[2:3]
    zero = jnp.zeros_like(w0)
    w0 = w0 + jnp.where(i1 == i0, w1, zero) + jnp.where(i2 == i0, w2, zero)
    w1 = w1 + jnp.where(i2 == i1, w2, zero)
    rows = REACH // 16
    iota = lax.broadcasted_iota(jnp.int32, (rows, 16, BLOCK), 0) * 16 + lax.broadcasted_iota(
        jnp.int32, (rows, 16, BLOCK), 1
    )
    iota = iota.astype(jnp.int16)
    parts = []
    for s in range(CHUNK // BLOCK):
        cols = slice(s * BLOCK, (s + 1) * BLOCK)
        base = s * BLOCK // RATIO

        def wide(x, kind):
            return jnp.broadcast_to(x[:, cols], (16, BLOCK)).astype(kind)[None]

        table = jnp.zeros((1, 16, BLOCK), BF16)
        for index, value in ((i2, w2), (i1, w1), (i0, w0)):
            table = jnp.where(wide(index - base, jnp.int16) == iota, wide(value, BF16), table)
        pieces = [table.reshape(REACH, BLOCK)]
        if base:
            pieces.insert(0, jnp.zeros((base, BLOCK), BF16))
        if base + REACH < WIN:
            pieces.append(jnp.zeros((WIN - base - REACH, BLOCK), BF16))
        parts.append(jnp.concatenate(pieces, axis=0))
    return jnp.concatenate(parts, axis=1)


def is_flipped():
    return (lax.axis_index("space") & 1) == 1


def spread_kernel(steps, done, chunks, *refs):
    first, last = done == 0, done + steps == chunks
    if first:
        anom_hbm, incr_hbm, index_hbm, weight_hbm, nbr_hbm = refs[:5]
        table_ref, out_ref, carry_ref = refs[5:8]
        anom_ref, incr_ref, index_ref, weight_ref, nbr_ref = refs[8:13]
        anom_sem, incr_sem, some_sem = refs[13:]
    else:
        anom_ref, incr_ref, index_ref, weight_ref, carry_in = refs[:5]
        table_ref, out_ref = refs[6:8]
        carry_ref = refs[-1]
    flip = is_flipped()

    def chunk_of(step):
        return jnp.where(flip, chunks - 1 - step, step)

    def lanes(c):
        return pl.ds(pl.multiple_of(c * CHUNK, CHUNK), CHUNK)

    if first:
        copies = [
            pltpu.make_async_copy(source, target, some_sem.at[k])
            for k, (source, target) in enumerate(
                ((index_hbm, index_ref), (weight_hbm, weight_ref), (nbr_hbm, nbr_ref))
            )
        ]
        columns = []
        for k, (begin, end) in enumerate(((0, steps), (steps, chunks))):
            low = jnp.where(flip, chunks - end, begin)
            here = pl.ds(pl.multiple_of(low * CHUNK, CHUNK), (end - begin) * CHUNK)
            columns.append(
                (
                    pltpu.make_async_copy(
                        anom_hbm.at[:, :, here], anom_ref.at[:, :, here], anom_sem.at[k]
                    ),
                    pltpu.make_async_copy(
                        incr_hbm.at[:, here], incr_ref.at[:, here], incr_sem.at[k]
                    ),
                )
            )
        for copy in (*copies[:2], *columns[0], *columns[1], copies[2]):
            copy.start()
        acc0 = acc1 = jnp.zeros(carry_ref.shape[1:], F32)
        for copy in copies[:2]:
            copy.wait()
    else:
        acc0, acc1 = carry_in[0], carry_in[1]
    rows = anom_ref.shape[0] * anom_ref.shape[1]
    total = out_ref.shape[0]

    def table_of(i):
        c = chunk_of(done + i)
        table = build_table(index_ref[:, lanes(c)] - c * BLOCK, weight_ref[:, lanes(c)])
        table_ref[c] = table
        return table

    before = steps if first else 0
    if first:
        for i in range(before):
            table_of(i)
        for copy in columns[0]:
            copy.wait()
    for i in range(steps):
        c = chunk_of(done + i)
        table = table_ref[c] if i < before else table_of(i)
        weighted = (anom_ref[:, :, lanes(c)].astype(F32) * incr_ref[:, lanes(c)][None]).astype(BF16)
        window = lax.dot_general(
            table,
            weighted.reshape(rows, CHUNK),
            (((1,), (1,)), ((), ())),
            preferred_element_type=F32,
        )
        near, mid, far = window[:BLOCK], window[BLOCK : 2 * BLOCK], window[2 * BLOCK :]
        ready = acc0 + jnp.where(flip, far, near)
        out_ref[jnp.where(flip, total - 1 - i, i)] = ready.T.astype(BF16)
        acc0 = acc1 + mid
        acc1 = jnp.where(flip, near, far)
    if last:
        out_ref[jnp.where(flip, 1, steps)] = acc0.T.astype(BF16)
        out_ref[jnp.where(flip, 0, steps + 1)] = acc1.T.astype(BF16)
    else:
        carry_ref[0] = acc0
        carry_ref[1] = acc1
    if first:
        for copy in (*columns[1], copies[2]):
            copy.wait()


def spread_first_call(steps, increment, anomalies, index, weight, neighbours):
    members, fields, columns = anomalies.shape
    rows = members * fields
    chunks = columns // CHUNK
    return call(
        functools.partial(spread_kernel, steps, 0, chunks),
        [ANY] * 5,
        [IN_VMEM] * 7 + [IN_SMEM],
        [
            VMEM((chunks, WIN, CHUNK), BF16),
            jax.ShapeDtypeStruct((steps, rows, BLOCK), BF16),
            VMEM((2, BLOCK, rows), F32),
            VMEM(anomalies.shape, BF16),
            VMEM(increment.shape, F32),
            VMEM(index.shape, jnp.int32),
            VMEM(weight.shape, F32),
            pltpu.SMEM(neighbours.shape, jnp.int32),
        ],
        [
            pltpu.SemaphoreType.DMA((2,)),
            pltpu.SemaphoreType.DMA((2,)),
            pltpu.SemaphoreType.DMA((3,)),
        ],
    )(*(in_hbm(x) for x in (anomalies, increment, index, weight, neighbours)))


def spread_more_call(done, steps, table, carry, columns):
    chunks = table.shape[0]
    rows = carry.shape[2]
    last = done + steps == chunks
    out_shape = [
        VMEM(table.shape, BF16),
        jax.ShapeDtypeStruct((steps + 2 * last, rows, BLOCK), BF16),
    ]
    if not last:
        out_shape.append(VMEM(carry.shape, F32))
    return call(
        functools.partial(spread_kernel, steps, done, chunks),
        [IN_VMEM] * 6,
        [IN_VMEM] * len(out_shape),
        out_shape,
        [],
        {5: 0},
    )(*columns, carry, table)


def convolve(wide_ref, tiles_ref, nbr_ref, b):
    count = tiles_ref.shape[1]
    picked = jnp.concatenate([wide_ref[nbr_ref[n, b]] for n in range(count)], axis=1)
    weights = tiles_ref[b].reshape(count * BLOCK, BLOCK)
    return jnp.dot(picked, weights, preferred_element_type=F32).astype(BF16)


def edge_early_kernel(
    nbr_ref, own_a, own_near, own_far, got_a, tiles_ref, wide_ref, smooth_ref, edge_ref
):
    half = own_a.shape[0]
    near = own_near.shape[0]
    reach = half - 1
    blocks = tiles_ref.shape[0]
    top = blocks + reach
    flip = is_flipped()

    @pl.when(jnp.logical_not(flip))
    def _():
        wide_ref[reach - 1 : reach - 1 + near] = own_near[...]
        wide_ref[reach - 1 + near : reach - 1 + half] = own_far[...]
        wide_ref[reach - 1 + half : top - 1] = own_a[0 : half - 2]
        wide_ref[top - 1 : top + 1] = (
            got_a[0:2].astype(F32) + own_a[half - 2 : half].astype(F32)
        ).astype(BF16)
        wide_ref[top + 1 : top + reach] = got_a[2:half]

    @pl.when(flip)
    def _():
        wide_ref[0 : reach - 1] = got_a[0 : reach - 1]
        wide_ref[reach - 1 : reach + 1] = (
            got_a[reach - 1 : reach + 1].astype(F32) + own_a[0:2].astype(F32)
        ).astype(BF16)
        wide_ref[reach + 1 : reach - 1 + half] = own_a[2:half]
        wide_ref[reach - 1 + half : top + 1 - near] = own_far[...]
        wide_ref[top + 1 - near : top + 1] = own_near[...]

    b = jnp.where(flip, 0, blocks - 1)
    edge = convolve(wide_ref, tiles_ref, nbr_ref, b)
    smooth_ref[b + 1] = edge
    edge_ref[...] = edge


def edge_late_kernel(
    nbr_ref, got_far, tiles_ref, wide_in, smooth_in, wide_ref, smooth_ref, edge_ref
):
    far = got_far.shape[0]
    blocks = tiles_ref.shape[0]
    flip = is_flipped()
    wide_ref[pl.ds(jnp.where(flip, wide_ref.shape[0] - far, 0), far)] = there(got_far[...])
    b = jnp.where(flip, blocks - 1, 0)
    edge = convolve(wide_ref, tiles_ref, nbr_ref, b)
    smooth_ref[b + 1] = edge
    edge_ref[...] = edge


def back_chunk(smooth_ref, table_ref, anom_ref, out_ref, c):
    shares = out_ref.shape[0]
    per = table_ref.shape[0] // shares
    lhs = jnp.concatenate([smooth_ref[c], smooth_ref[c + 1], smooth_ref[c + 2]], axis=1)
    returned = jnp.dot(lhs, table_ref[c], preferred_element_type=F32)
    here = pl.ds(pl.multiple_of(c * CHUNK, CHUNK), CHUNK)
    anom = anom_ref[:, :, here].astype(F32)
    value = jnp.sum(anom * returned.reshape(anom.shape), axis=0)
    place = lax.div(c, per) - lax.axis_index("mem")
    place = jnp.where(place < 0, place + shares, place)
    lane = pl.multiple_of(lax.rem(c, per) * CHUNK, CHUNK)
    out_ref[place, :, pl.ds(lane, CHUNK)] = value.astype(BF16)


def there(value):
    return jnp.where(is_present(), value, jnp.zeros_like(value))


def early_kernel(
    steps,
    nbr_ref,
    got_near,
    wide_in,
    tiles_ref,
    table_ref,
    anom_ref,
    smooth_in,
    wide_ref,
    smooth_ref,
    out_ref,
):
    blocks = tiles_ref.shape[0]
    near = got_near.shape[0]
    half = blocks - steps - 1
    reach = half - 1
    top = blocks + reach
    flip = is_flipped()
    start = jnp.where(flip, 1, blocks - 1 - steps)
    for i in range(steps):
        smooth_ref[start + i + 1] = convolve(wide_ref, tiles_ref, nbr_ref, start + i)

    @pl.when(jnp.logical_not(flip))
    def _():
        wide_ref[half - near : reach - 1] = there(got_near[0 : near - 2])
        both = wide_ref[reach - 1 : reach + 1].astype(F32) + there(got_near[near - 2 :].astype(F32))
        wide_ref[reach - 1] = there(both[0]).astype(BF16)
        wide_ref[reach] = both[1].astype(BF16)

    @pl.when(flip)
    def _():
        both = wide_ref[top - 1 : top + 1].astype(F32) + there(got_near[0:2].astype(F32))
        wide_ref[top - 1] = both[0].astype(BF16)
        wide_ref[top] = there(both[1]).astype(BF16)
        wide_ref[top + 1 : top - 1 + near] = there(got_near[2:near])

    start = jnp.where(flip, blocks - half, half - near)
    for i in range(near):
        smooth_ref[start + i + 1] = convolve(wide_ref, tiles_ref, nbr_ref, start + i)
    start = jnp.where(flip, 1, half - near + 1)
    for i in range(steps - 1 + near):
        back_chunk(smooth_ref, table_ref, anom_ref, out_ref, start + i)


def late_kernel(
    steps,
    nbr_ref,
    halo_ref,
    wide_ref,
    tiles_ref,
    table_ref,
    anom_ref,
    smooth_in,
    out_in,
    smooth_ref,
    out_ref,
    main_ref,
):
    blocks = tiles_ref.shape[0]
    flip = is_flipped()
    start = jnp.where(flip, blocks - 1 - steps, 1)
    for i in range(steps):
        smooth_ref[start + i + 1] = convolve(wide_ref, tiles_ref, nbr_ref, start + i)
    start = jnp.where(flip, blocks - 2 - steps, 1)
    smooth_ref[jnp.where(flip, 0, blocks + 1)] = halo_ref[...]
    back_chunk(smooth_ref, table_ref, anom_ref, out_ref, jnp.where(flip, 0, blocks - 1))
    for i in range(steps + 1):
        back_chunk(smooth_ref, table_ref, anom_ref, out_ref, start + i)
    width = main_ref.shape[1]
    here = pl.ds(pl.multiple_of(jnp.where(flip, 0, CHUNK), CHUNK), width)
    main_ref[...] = out_ref[1, :, here]


def last_kernel(
    halo_ref, table_ref, anom_ref, smooth_in, out_in, smooth_ref, out_ref, edge_ref
):
    blocks = table_ref.shape[0]
    flip = is_flipped()
    halo = halo_ref[...]
    smooth_ref[jnp.where(flip, blocks + 1, 0)] = jnp.where(is_present(), halo, jnp.zeros_like(halo))
    back_chunk(smooth_ref, table_ref, anom_ref, out_ref, jnp.where(flip, blocks - 1, 0))
    _, _, columns = out_ref.shape
    here = pl.ds(pl.multiple_of(jnp.where(flip, columns - CHUNK, 0), CHUNK), CHUNK)
    edge_ref[...] = out_ref[1, :, here]


def edge_early_call(neighbours, own_a, own_near, own_far, got_a, tiles):
    blocks = tiles.shape[0]
    half, rows, _ = own_a.shape
    return call(
        edge_early_kernel,
        [IN_SMEM] + [IN_VMEM] * 5,
        [IN_VMEM] * 3,
        [
            VMEM((blocks + 2 * half - 2, rows, BLOCK), BF16),
            VMEM((blocks + 2, rows, BLOCK), BF16),
            jax.ShapeDtypeStruct((rows, BLOCK), BF16),
        ],
        [],
    )(neighbours, own_a, own_near, own_far, got_a, tiles)


def edge_late_call(neighbours, got_far, tiles, wide, smooth):
    _, rows, _ = got_far.shape
    return call(
        edge_late_kernel,
        [IN_SMEM] + [IN_VMEM] * 4,
        [IN_VMEM] * 3,
        [
            VMEM(wide.shape, BF16),
            VMEM(smooth.shape, BF16),
            jax.ShapeDtypeStruct((rows, BLOCK), BF16),
        ],
        [],
        {3: 0, 4: 1},
    )(neighbours, got_far, tiles, wide, smooth)


def early_call(steps, shares, neighbours, got_near, wide, tiles, table, anom, smooth):
    _, fields, columns = anom.shape
    return call(
        functools.partial(early_kernel, steps),
        [IN_SMEM] + [IN_VMEM] * 6,
        [IN_VMEM] * 3,
        [
            VMEM(wide.shape, BF16),
            VMEM(smooth.shape, BF16),
            VMEM((shares, fields, columns // shares), BF16),
        ],
        [],
        {2: 0, 6: 1},
    )(neighbours, got_near, wide, tiles, table, anom, smooth)


def late_call(steps, neighbours, halo, wide, tiles, table, anom, smooth, out):
    return call(
        functools.partial(late_kernel, steps),
        [IN_SMEM] + [IN_VMEM] * 7,
        [IN_VMEM] * 3,
        [
            VMEM(smooth.shape, BF16),
            VMEM(out.shape, BF16),
            jax.ShapeDtypeStruct((out.shape[1], out.shape[2] - CHUNK), BF16),
        ],
        [],
        {6: 0, 7: 1},
    )(neighbours, halo, wide, tiles, table, anom, smooth, out)


def last_call(halo, table, anom, smooth, out):
    return call(
        last_kernel,
        [IN_VMEM] * 5,
        [IN_VMEM] * 3,
        [
            VMEM(smooth.shape, BF16),
            jax.ShapeDtypeStruct(out.shape, BF16),
            jax.ShapeDtypeStruct((out.shape[1], CHUNK), BF16),
        ],
        [],
        {3: 0, 4: 1},
    )(halo, table, anom, smooth, out)


def swaps(count, shares):
    inner, outer = [], []
    for i in range(count):
        far = i + 1 if i % 2 else i - 1
        for m in range(shares):
            here = i * shares + m
            inner.append((here, (i ^ 1) * shares + m))
            outer.append((here, far * shares + m if 0 <= far < count else i * shares + (m ^ 1)))
    return inner, outer


def swap(value, pairs):
    return lax.ppermute(value, ("space", "mem"), pairs)


def pass_on(value, shift, shares):
    return lax.ppermute(value, "mem", [(i, (i + shift) % shares) for i in range(shares)])


def shards(increment, anomalies, interp_index, interp_weight, neighbour_blocks, tiles):
    members, _, columns = anomalies.shape
    chunks = columns // CHUNK
    count = lax.axis_size("space")
    shares = lax.axis_size("mem")
    assert count % 2 == 0 and shares % 2 == 0 and chunks > shares
    inner, outer = swaps(count, shares)
    head = chunks // 2 + 1
    table, own_near, carry, anom, *columns_here, neighbours = spread_first_call(
        NEAR, increment, anomalies, interp_index, interp_weight, neighbour_blocks
    )
    columns_here = (anom, *columns_here)
    got_near = swap(own_near, outer)
    table, own_far, carry = spread_more_call(NEAR, head - NEAR, table, carry, columns_here)
    got_far = swap(own_far, outer)
    table, own_a = spread_more_call(head, chunks - head, table, carry, columns_here)
    got_a = swap(own_a, inner)
    early = chunks - head - 1
    wide, smooth, edge_a = edge_early_call(
        neighbours, own_a, own_near, own_far, got_a, tiles
    )
    halo_a = swap(edge_a, inner)
    wide, smooth, out = early_call(
        early, shares, neighbours, got_near, wide, tiles, table, anom, smooth
    )
    wide, smooth, edge_b = edge_late_call(neighbours, got_far, tiles, wide, smooth)
    halo_b = swap(edge_b, outer)
    smooth, out, main = late_call(
        head - 1 - NEAR, neighbours, halo_a, wide, tiles, table, anom, smooth, out
    )
    half = 1
    main = pass_on(main, half, shares)
    _, pieces, edge = last_call(halo_b, table, anom, smooth, out)
    total = pieces[0].astype(F32)
    for shift in range(1, shares):
        piece = edge if shift == half else pieces[shift]
        got = pass_on(piece, shift, shares)
        if shift == half:
            flip = is_flipped()
            got = jnp.where(
                flip,
                jnp.concatenate([main, got], axis=1),
                jnp.concatenate([got, main], axis=1),
            )
        total = total + got.astype(F32)
    return total / (members * shares - 1)


def solution(mesh):
    in_specs = (
        P(None, "space"),
        P("mem", None, "space"),
        P(None, "space"),
        P(None, "space"),
        P(None, "space"),
        P("space", None, None, None),
    )
    out_specs = P(None, ("space", "mem"))
    return jax.shard_map(shards, mesh=mesh, in_specs=in_specs, out_specs=out_specs, check_vma=False)
```
